32 devices in a mesh: dp: 4 (over y, core), ctx: 4 (over z), tp: 2 (over x).
Axes of the slice: x: 2, y: 2, z: 4, core: 2. Of those that a mesh axis runs over, the one named last changes fastest.
Arguments:
- block_input: bfloat16 [8, 2048, 896], P('dp', 'ctx'), may hold values from -6 to 6
- positions: int32 [8, 2048], P('dp', 'ctx'), may hold values from 0 to 1535, as said below
- gain_attn: float32 [896], replicated, may hold values from 0.25 to 1.75
- w_qkv: bfloat16 [896, 2, 576], P(None, 'tp'), may hold values from -0.2893103 to 0.2893103, as said below
- b_qkv: float32 [2, 576], P('tp'), may hold values from -3 to 3
- w_out: bfloat16 [2, 448, 896], P('tp'), may hold values from -3 to 3
- gain_mlp: float32 [896], replicated, may hold values from 0.25 to 1.75
- w_gate: bfloat16 [896, 4864], P(None, 'tp'), may hold values from -0.1875 to 0.1875
- w_up: bfloat16 [896, 4864], P(None, 'tp'), may hold values from -0.1875 to 0.1875
- w_down: bfloat16 [4864, 896], P('tp'), may hold values from -0.625 to 0.625
- cotangent: bfloat16 [8, 2048, 896], P('dp', 'ctx'), may hold values from -6 to 6
Outputs:
- output: bfloat16 [8, 2048, 896], P('dp', 'ctx')
- grad_input: float32 [8, 2048, 896], P('dp', 'ctx')
- grad_gain_attn: float32 [896], P('dp')
- grad_qkv: float32 [896, 2, 576], P('dp', 'tp')
- grad_bias: float32 [2, 576], P('tp', 'dp')
- grad_out: float32 [2, 448, 896], P('tp', None, 'dp')
- grad_gain_mlp: float32 [896], P('dp')
- grad_gate: float32 [896, 4864], P('dp', 'tp')
- grad_up: float32 [896, 4864], P('dp', 'tp')
- grad_down: float32 [4864, 896], P('tp', 'dp')
The draws below stay inside these ranges and needn't reach their ends.
Inputs may be any that keep to these rules, and one draw needn't show every extreme that they name: Each sequence holds two documents; the second starts at an index between 512 and 1536 drawn per sequence, in the first sequence exactly at 512; the position restarts at 0 there, and within a document positions count up by one. `w_qkv`: independent entries.
All inputs are finite; a program needn't handle non-finite values.
Results may differ from the reference program's by a relative error of at most 0.03.
The reference program's roundings to bfloat16 on the way (of `hidden_one`, `attended`, `hidden_two`, `activated`, `grad_middle_b`, `grad_attended`, `grad_scores` and `grad_joined_b`) count: a program that leaves them out, or rounds other values in their place, can miss the bound.
Values may be sent and summed in bfloat16 or wider, within the bound.
A program may use at most 256 MiB of HBM per device.

```python
import math
import jax
import jax.numpy as jnp
from jax import lax

D = 896
KVH = 2
HD = 64
FF = 4864
GROUP = 7
QKV = 576
LEN = 2048
BATCH = 8


def draw_positions(key, part):
    boundary = jax.random.randint(key, (BATCH, 1), LEN // 4, 3 * LEN // 4, dtype=jnp.int32)
    row_index = jnp.arange(BATCH, dtype=jnp.int32)[:, None]
    boundary = jnp.where(row_index == 0, LEN // 4, boundary).astype(jnp.int32)
    index = jnp.arange(LEN, dtype=jnp.int32)[None, :]
    return jnp.where(index < boundary, index, index - boundary).astype(jnp.int32)


def draw_w_qkv(key, part):
    spread = D ** (-0.5)
    return (jax.random.uniform(key, (D, KVH, QKV), jnp.float32, -1.0, 1.0) * 3.0 ** 0.5 * spread).astype(jnp.bfloat16)


def levels(rng, shape, cuts, smallest, top_value):
    loudness, own = 1.0, jax.random.fold_in(rng, 6)
    for position, blocks in cuts:
        draws = jnp.exp(jax.random.uniform(jax.random.fold_in(own, position), (blocks,), jnp.float32, smallest / len(cuts), top_value / len(cuts)))
        loudness = loudness * jnp.repeat(draws, shape[position] // blocks).reshape([-1 if axis == position else 1 for axis in range(len(shape))])
    return loudness


def gaussian(rng, shape, scale, limit, split=(), kind=jnp.bfloat16):
    array = scale * jax.random.normal(rng, shape, jnp.float32)
    if split:
        array = array * levels(rng, shape, split, -0.22, 0.18)
    return jnp.clip(array, -limit, limit).astype(kind)


def setup_inputs(seed: int = 0) -> dict:
    arg_keys = jax.random.split(jax.random.key(seed), 12)
    return {
        "block_input": gaussian(arg_keys[0], (BATCH, LEN, D), 1.0, 6.0, ((0, 4), (1, 4))),
        "positions": draw_positions(jax.random.fold_in(arg_keys[11], 71), 0),
        "gain_attn": jnp.clip(1.0 + 0.15 * jax.random.normal(arg_keys[2], (D,), jnp.float32), 0.25, 1.75),
        "w_qkv": draw_w_qkv(jax.random.fold_in(arg_keys[11], 71), 0),
        "b_qkv": gaussian(arg_keys[4], (KVH, QKV), 0.5, 3.0, ((0, 2),), jnp.float32),
        "w_out": gaussian(arg_keys[5], (KVH, GROUP * HD, D), (HD // 16) ** -0.5, 3.0, ((0, 2),)),
        "gain_mlp": jnp.clip(1.0 + 0.15 * jax.random.normal(arg_keys[6], (D,), jnp.float32), 0.25, 1.75),
        "w_gate": gaussian(arg_keys[7], (D, FF), D ** -0.5, 0.1875, ((1, 2),)),
        "w_up": gaussian(arg_keys[8], (D, FF), D ** -0.5, 0.1875, ((1, 2),)),
        "w_down": gaussian(arg_keys[9], (FF, D), (FF // 64) ** -0.5, 0.625, ((0, 2),)),
        "cotangent": gaussian(arg_keys[10], (BATCH, LEN, D), 1.0, 6.0, ((0, 4), (1, 4))),
    }


EPS = 1e-06
THETA = 1000000.0
SCALE = 0.125

def rounded(values):
    return lax.optimization_barrier(values.astype(jnp.bfloat16))

def inverse_rms(values):
    return lax.rsqrt(lax.optimization_barrier(jnp.mean(values * values, axis=-1, keepdims=True)) + EPS)

def rotary(positions, width):
    half = width // 2
    freq = THETA ** (-(jnp.arange(half, dtype=jnp.float32) * 2.0) / width)
    angle = positions.astype(jnp.float32)[..., None] * freq
    return (jnp.cos(angle), jnp.sin(angle))

def rotate(values, cosine, sine):
    half = values.shape[-1] // 2
    first, second = (values[..., :half], values[..., half:])
    return jnp.concatenate([first * cosine - second * sine, second * cosine + first * sine], axis=-1)

def unrotate(grads, cosine, sine):
    half = grads.shape[-1] // 2
    first, second = (grads[..., :half], grads[..., half:])
    return jnp.concatenate([first * cosine + second * sine, second * cosine - first * sine], axis=-1)

def norm_back(grad_h, normed, scale, gain):
    upstream = grad_h * gain
    inner = lax.optimization_barrier(jnp.mean(upstream * normed, axis=-1, keepdims=True))
    return scale * (upstream - normed * inner)

def one_sequence(params, block, positions, cotangent):
    gain_attn, w_qkv, b_qkv, w_out, gain_mlp, w_gate, w_up, w_down = params
    qsize = math.gcd(LEN, 512)
    count = LEN // qsize
    heads_width = GROUP * HD
    inputs = block.astype(jnp.float32)
    scale_one = inverse_rms(inputs)
    normed_one = inputs * scale_one
    hidden_one = rounded(normed_one * gain_attn)
    joined = jnp.einsum('td,dhe->the', hidden_one.astype(jnp.float32), w_qkv.astype(jnp.float32)) + b_qkv
    cosine, sine = rotary(positions, HD)
    queries = rounded(rotate(joined[:, :, :heads_width].reshape(LEN, KVH, GROUP, HD), cosine[:, None, None, :], sine[:, None, None, :]))
    keys = rounded(rotate(joined[:, :, heads_width:heads_width + HD], cosine[:, None, :], sine[:, None, :]))
    values = rounded(joined[:, :, heads_width + HD:])
    query_f = queries.astype(jnp.float32)
    key_f = keys.astype(jnp.float32)
    value_f = values.astype(jnp.float32)
    index = jnp.arange(LEN, dtype=jnp.int32)
    first = index - positions.astype(jnp.int32)

    def allowed_for(start):
        rows = start + jnp.arange(qsize, dtype=jnp.int32)
        lowest = lax.dynamic_slice_in_dim(first, start, qsize)
        return (index[None, :] <= rows[:, None]) & (index[None, :] >= lowest[:, None])

    def forward_block(turn):
        start = turn * qsize
        qblock = lax.dynamic_slice_in_dim(query_f, start, qsize, 0)
        scores = jnp.einsum('qhgd,khd->hgqk', qblock, key_f) * SCALE
        allowed = allowed_for(start)[None, None]
        top = lax.optimization_barrier(jnp.max(jnp.where(allowed, scores, -jnp.inf), axis=-1, keepdims=True))
        weights = jnp.where(allowed, jnp.exp(scores - top), 0.0)
        total = lax.optimization_barrier(jnp.sum(weights, axis=-1, keepdims=True))
        mixed = jnp.einsum('hgqk,khd->hgqd', rounded(weights).astype(jnp.float32), value_f) / total
        return (rounded(jnp.transpose(mixed, (2, 0, 1, 3))), (top + jnp.log(total))[..., 0])
    attended_blocks, lse_blocks = lax.map(forward_block, jnp.arange(count, dtype=jnp.int32))
    attended = attended_blocks.reshape(LEN, KVH, heads_width)
    attended_f = attended.astype(jnp.float32)
    middle = inputs + jnp.einsum('the,hed->td', attended_f, w_out.astype(jnp.float32))
    scale_two = inverse_rms(middle)
    normed_two = middle * scale_two
    hidden_two = rounded(normed_two * gain_mlp)
    gate = jnp.dot(hidden_two, w_gate, preferred_element_type=jnp.float32)
    up = jnp.dot(hidden_two, w_up, preferred_element_type=jnp.float32)
    sigma = jax.nn.sigmoid(gate)
    activated = rounded(gate * sigma * up)
    output = (middle + jnp.dot(activated, w_down, preferred_element_type=jnp.float32)).astype(jnp.bfloat16)
    grad_act = jnp.dot(cotangent, w_down.T, preferred_element_type=jnp.float32)
    grad_down = jnp.dot(activated.T, cotangent, preferred_element_type=jnp.float32)
    grad_gate_in = rounded(grad_act * up * sigma * (1.0 + gate * (1.0 - sigma)))
    grad_up_in = rounded(grad_act * gate * sigma)
    grad_gate = jnp.dot(hidden_two.T, grad_gate_in, preferred_element_type=jnp.float32)
    grad_up = jnp.dot(hidden_two.T, grad_up_in, preferred_element_type=jnp.float32)
    back_two = jnp.dot(grad_gate_in, w_gate.T, preferred_element_type=jnp.float32) + jnp.dot(grad_up_in, w_up.T, preferred_element_type=jnp.float32)
    grad_gain_mlp = lax.optimization_barrier(jnp.sum(back_two * normed_two, axis=0))
    grad_middle = cotangent.astype(jnp.float32) + norm_back(back_two, normed_two, scale_two, gain_mlp)
    grad_middle_b = rounded(grad_middle)
    grad_out = jnp.einsum('the,td->hed', attended_f, grad_middle_b.astype(jnp.float32))
    grad_attended = rounded(jnp.einsum('td,hed->the', grad_middle_b.astype(jnp.float32), w_out.astype(jnp.float32)))
    grad_att_f = grad_attended.astype(jnp.float32).reshape(LEN, KVH, GROUP, HD)
    row_terms = lax.optimization_barrier(jnp.sum(grad_att_f * attended_f.reshape(LEN, KVH, GROUP, HD), axis=-1))

    def backward_block(carry, item):
        grad_keys, grad_values = carry
        turn, lse_block = item
        start = turn * qsize
        qblock = lax.dynamic_slice_in_dim(query_f, start, qsize, 0)
        gblock = lax.dynamic_slice_in_dim(grad_att_f, start, qsize, 0)
        rblock = lax.dynamic_slice_in_dim(row_terms, start, qsize, 0)
        scores = jnp.einsum('qhgd,khd->hgqk', qblock, key_f) * SCALE
        allowed = allowed_for(start)[None, None]
        probs = jnp.where(allowed, jnp.exp(scores - lse_block[..., None]), 0.0)
        grad_probs = jnp.einsum('qhgd,khd->hgqk', gblock, value_f)
        grad_scores = rounded(probs * (grad_probs - jnp.transpose(rblock, (1, 2, 0))[..., None])).astype(jnp.float32)
        grad_q = jnp.einsum('hgqk,khd->qhgd', grad_scores, key_f) * SCALE
        grad_keys = grad_keys + jnp.einsum('hgqk,qhgd->khd', grad_scores, qblock) * SCALE
        grad_values = grad_values + jnp.einsum('hgqk,qhgd->khd', rounded(probs).astype(jnp.float32), gblock)
        return ((grad_keys, grad_values), grad_q)
    empty = jnp.zeros((LEN, KVH, HD), jnp.float32)
    carried, grad_q_blocks = lax.scan(backward_block, (empty, empty), (jnp.arange(count, dtype=jnp.int32), lse_blocks))
    grad_keys, grad_values = carried
    grad_queries = grad_q_blocks.reshape(LEN, KVH, GROUP, HD)
    grad_joined = jnp.concatenate([unrotate(grad_queries, cosine[:, None, None, :], sine[:, None, None, :]).reshape(LEN, KVH, heads_width), unrotate(grad_keys, cosine[:, None, :], sine[:, None, :]), grad_values], axis=-1)
    grad_bias = lax.optimization_barrier(jnp.sum(grad_joined, axis=0))
    grad_joined_b = rounded(grad_joined).astype(jnp.float32)
    grad_qkv = jnp.einsum('td,the->dhe', hidden_one.astype(jnp.float32), grad_joined_b)
    back_one = jnp.einsum('the,dhe->td', grad_joined_b, w_qkv.astype(jnp.float32))
    grad_gain_attn = lax.optimization_barrier(jnp.sum(back_one * normed_one, axis=0))
    grad_input = grad_middle + norm_back(back_one, normed_one, scale_one, gain_attn)
    terms = (grad_gain_attn, grad_qkv, grad_bias, grad_out, grad_gain_mlp, grad_gate, grad_up, grad_down)
    return (output, grad_input, terms)

def reference(block_input, positions, gain_attn, w_qkv, b_qkv, w_out, gain_mlp, w_gate, w_up, w_down, cotangent):
    params = (gain_attn, w_qkv, b_qkv, w_out, gain_mlp, w_gate, w_up, w_down)
    start_grads = (jnp.zeros(gain_attn.shape, jnp.float32), jnp.zeros(w_qkv.shape, jnp.float32), jnp.zeros(b_qkv.shape, jnp.float32), jnp.zeros(w_out.shape, jnp.float32), jnp.zeros(gain_mlp.shape, jnp.float32), jnp.zeros(w_gate.shape, jnp.float32), jnp.zeros(w_up.shape, jnp.float32), jnp.zeros(w_down.shape, jnp.float32))

    def step(grads, item):
        block, pos, cot = item
        output, grad_input, terms = one_sequence(params, block, pos, cot)
        return (jax.tree.map(jnp.add, grads, terms), (output, grad_input))
    grads, produced = lax.scan(step, start_grads, (block_input, positions, cotangent))
    return (produced[0], produced[1], grads[0], grads[1], grads[2], grads[3], grads[4], grads[5], grads[6], grads[7])
```

```python
import math

import jax
import jax.numpy as jnp
from jax import lax
from jax.sharding import PartitionSpec as P

HD = 64


EPS = 1e-06
THETA = 1000000.0
SCALE = 0.125
NEGATIVE = -1e30


def inverse_rms(values):
    return lax.rsqrt(jnp.mean(values * values, axis=-1, keepdims=True) + EPS)


def rotary(positions, width):
    half = width // 2
    freq = THETA ** (-(jnp.arange(half, dtype=jnp.float32) * 2.0) / width)
    angle = positions.astype(jnp.float32)[..., None] * freq
    return (jnp.cos(angle), jnp.sin(angle))


def rotate(values, cosine, sine):
    half = values.shape[-1] // 2
    first, second = (values[..., :half], values[..., half:])
    return jnp.concatenate(
        [first * cosine - second * sine, second * cosine + first * sine], axis=-1
    )


def unrotate(grads, cosine, sine):
    half = grads.shape[-1] // 2
    first, second = (grads[..., :half], grads[..., half:])
    return jnp.concatenate(
        [first * cosine + second * sine, second * cosine - first * sine], axis=-1
    )


def norm_back(grad_h, normed, scale, gain):
    upstream = grad_h * gain
    inner = jnp.mean(upstream * normed, axis=-1, keepdims=True)
    return scale * (upstream - normed * inner)


def to_bf16(values):
    return values.astype(jnp.bfloat16)


def tp_other(values):
    return lax.ppermute(values, "tp", [(0, 1), (1, 0)])


def tp_sum(values):
    mine = to_bf16(values)
    return mine.astype(jnp.float32) + tp_other(mine).astype(jnp.float32)


def core_other(values):
    pairs = [(i, i ^ 1) for i in range(lax.axis_size("dp"))]
    return lax.ppermute(values, "dp", pairs)


def earlier(values, shift):
    n = lax.axis_size("ctx")
    return lax.ppermute(values, "ctx", [(i, i + shift) for i in range(n - shift)])


def later(values, shift):
    n = lax.axis_size("ctx")
    return lax.ppermute(values, "ctx", [(i + shift, i) for i in range(n - shift)])


def line_sum(part):
    n = lax.axis_size("ctx")
    half = n // 2
    me = lax.axis_index("ctx")
    for step in range(half - 1):
        pairs = [(step, step + 1), (n - 1 - step, n - 2 - step)]
        part = part + lax.ppermute(to_bf16(part), "ctx", pairs).astype(jnp.float32)
    mine = to_bf16(part)
    moved = lax.ppermute(mine, "ctx", [(half - 1, half), (half, half - 1)])
    total = to_bf16(mine.astype(jnp.float32) + moved.astype(jnp.float32))
    for step in reversed(range(half - 1)):
        pairs = [(step + 1, step), (n - 2 - step, n - 1 - step)]
        moved = lax.ppermute(total, "ctx", pairs)
        total = jnp.where((me == step) | (me == n - 1 - step), moved, total)
    return total.astype(jnp.float32)


def quarter_grads(make, wide):
    n_dp = lax.axis_size("dp")
    rows = n_dp // 2
    me = lax.axis_index("dp")
    row, core = me // 2, me % 2
    split = wide.reshape(wide.shape[0], rows, 2, wide.shape[1] // n_dp)
    mine = lax.dynamic_index_in_dim(split, core, 2, keepdims=False)
    theirs = core_other(lax.dynamic_index_in_dim(split, 1 - core, 2, keepdims=False))
    both = jnp.concatenate([mine, theirs], axis=0)

    def columns(which):
        return lax.dynamic_index_in_dim(both, which, 1, keepdims=False)

    total = None
    for shift in range(1, rows):
        part = to_bf16(make(columns((row + shift) % rows)))
        pairs = [(r * 2 + c, ((r + shift) % rows) * 2 + c) for r in range(rows) for c in range(2)]
        moved = lax.ppermute(part, "dp", pairs).astype(jnp.float32)
        total = moved if total is None else total + moved
    own = make(columns(row))
    return own if total is None else own + total


def both_cores(values):
    return jnp.concatenate([values, core_other(values)], axis=0)


def shards(
    block_input,
    positions,
    gain_attn,
    w_qkv,
    b_qkv,
    w_out,
    gain_mlp,
    w_gate,
    w_up,
    w_down,
    cotangent,
):
    seqs, tokens, _ = block_input.shape
    heads_width = w_out.shape[1]
    head = HD
    group = heads_width // head
    rows = tokens * group
    first_token = lax.axis_index("ctx") * tokens
    seq_tokens = tokens * lax.axis_size("ctx")
    proj_qkv = w_qkv[:, 0, :]
    proj_out = w_out[0]
    other_qkv = tp_other(proj_qkv)
    other_out = tp_other(proj_out)
    inputs = block_input.astype(jnp.float32)
    scale_one = inverse_rms(inputs)
    normed_one = inputs * scale_one
    hidden_one = (normed_one * gain_attn).astype(jnp.bfloat16)
    joined = (
        jnp.einsum("std,de->ste", hidden_one, proj_qkv, preferred_element_type=jnp.float32)
        + b_qkv[0]
    )
    cosine, sine = rotary(positions, head)
    queries = rotate(
        joined[..., :heads_width].reshape(seqs, tokens, group, head),
        cosine[:, :, None, :],
        sine[:, :, None, :],
    )
    queries = queries.astype(jnp.bfloat16).reshape(seqs, rows, head)
    keys = rotate(joined[..., heads_width : heads_width + head], cosine, sine)
    key_value = jnp.concatenate([keys, joined[..., heads_width + head :]], axis=-1).astype(
        jnp.bfloat16
    )
    gathered = jnp.zeros((seqs, seq_tokens, 2 * head), jnp.bfloat16)
    gathered = lax.dynamic_update_slice_in_dim(gathered, key_value, first_token, 1)
    n_ctx = lax.axis_size("ctx")
    for shift in range(1, n_ctx):
        place = (lax.axis_index("ctx") - shift) % n_ctx * tokens
        gathered = lax.dynamic_update_slice_in_dim(gathered, earlier(key_value, shift), place, 1)
    token_index = first_token + jnp.arange(tokens, dtype=jnp.int32)
    query_index = jnp.repeat(token_index, group)
    query_first = jnp.repeat(token_index[None, :] - positions, group, axis=1)
    query_last = first_token + tokens - 1

    def block_scores(key_block, key_start):
        scores = (
            jnp.einsum(
                "srd,skd->srk", queries, key_block[..., :head], preferred_element_type=jnp.float32
            )
            * SCALE
        )
        key_index = key_start + jnp.arange(key_block.shape[1], dtype=jnp.int32)
        allowed = (key_index[None, None, :] <= query_index[None, :, None]) & (
            key_index[None, None, :] >= query_first[:, :, None]
        )
        return (scores, allowed)

    def over_blocks(step_fn, carry, piece):
        size = math.gcd(piece.shape[1], 512)
        count = piece.shape[1] // size

        def one_block(turn, state):
            offset = turn * size
            key_block = lax.dynamic_slice_in_dim(piece, offset, size, 1)
            return lax.cond(
                offset <= query_last,
                lambda inner: step_fn(inner, key_block, offset),
                lambda inner: inner,
                state,
            )

        return lax.fori_loop(0, count, one_block, carry)

    def forward_step(state, key_block, key_start):
        top, total, accum = state
        scores, allowed = block_scores(key_block, key_start)
        new_top = jnp.maximum(top, jnp.max(jnp.where(allowed, scores, NEGATIVE), axis=-1))
        weights = jnp.where(allowed, jnp.exp(scores - new_top[..., None]), 0.0)
        factor = jnp.exp(top - new_top)
        total = total * factor + jnp.sum(weights, axis=-1)
        accum = accum * factor[..., None] + jnp.einsum(
            "srk,skd->srd",
            weights.astype(jnp.bfloat16),
            key_block[..., head:],
            preferred_element_type=jnp.float32,
        )
        return (new_top, total, accum)

    start_state = (
        jnp.full((seqs, rows), NEGATIVE, jnp.float32),
        jnp.zeros((seqs, rows), jnp.float32),
        jnp.zeros((seqs, rows, head), jnp.float32),
    )
    top, total, accum = over_blocks(
        forward_step, start_state, gathered
    )
    log_total = top + jnp.log(total)
    attended = (accum / total[..., None]).astype(jnp.bfloat16)
    attended_flat = attended.reshape(seqs, tokens, heads_width)
    attn_mine = jnp.einsum(
        "ste,ed->std", attended_flat, proj_out, preferred_element_type=jnp.float32
    )
    attn_other = jnp.einsum(
        "ste,ed->std", tp_other(attended_flat), other_out, preferred_element_type=jnp.float32
    )
    middle = inputs + (attn_mine + attn_other)
    scale_two = inverse_rms(middle)
    normed_two = middle * scale_two
    hidden_two = (normed_two * gain_mlp).astype(jnp.bfloat16)
    gate = jnp.einsum("std,df->stf", hidden_two, w_gate, preferred_element_type=jnp.float32)
    up = jnp.einsum("std,df->stf", hidden_two, w_up, preferred_element_type=jnp.float32)
    sigma = jax.nn.sigmoid(gate)
    activated = (gate * sigma * up).astype(jnp.bfloat16)
    mlp_part = jnp.einsum("stf,fd->std", activated, w_down, preferred_element_type=jnp.float32)
    output = (middle + tp_sum(mlp_part)).astype(jnp.bfloat16)
    grad_act = jnp.einsum("std,fd->stf", cotangent, w_down, preferred_element_type=jnp.float32)
    grad_gate_in = (grad_act * up * sigma * (1.0 + gate * (1.0 - sigma))).astype(jnp.bfloat16)
    grad_up_in = (grad_act * gate * sigma).astype(jnp.bfloat16)
    flat = seqs * tokens
    acts = both_cores(activated.reshape(flat, -1))
    gates = both_cores(grad_gate_in.reshape(flat, -1))
    ups = both_cores(grad_up_in.reshape(flat, -1))
    grad_down = quarter_grads(
        lambda cols: jnp.einsum("tf,td->fd", acts, cols, preferred_element_type=jnp.float32),
        cotangent.reshape(flat, -1),
    )
    hidden_flat = hidden_two.reshape(flat, -1)
    grad_gate = quarter_grads(
        lambda cols: jnp.einsum("td,tf->df", cols, gates, preferred_element_type=jnp.float32),
        hidden_flat,
    )
    grad_up = quarter_grads(
        lambda cols: jnp.einsum("td,tf->df", cols, ups, preferred_element_type=jnp.float32),
        hidden_flat,
    )
    grad_down = line_sum(grad_down)
    grad_gate = line_sum(grad_gate)
    grad_up = line_sum(grad_up)
    back_two = jnp.einsum("stf,df->std", grad_gate_in, w_gate, preferred_element_type=jnp.float32)
    back_two = back_two + jnp.einsum(
        "stf,df->std", grad_up_in, w_up, preferred_element_type=jnp.float32
    )
    back_two = tp_sum(back_two)
    grad_gain_mlp = jnp.sum(back_two * normed_two, axis=(0, 1))
    grad_middle = cotangent.astype(jnp.float32) + norm_back(
        back_two, normed_two, scale_two, gain_mlp
    )
    grad_middle_b = grad_middle.astype(jnp.bfloat16)
    att_both = both_cores(attended_flat.reshape(flat, -1))
    grad_out = quarter_grads(
        lambda cols: jnp.einsum("te,td->ed", att_both, cols, preferred_element_type=jnp.float32),
        grad_middle_b.reshape(flat, -1),
    )
    grad_out = line_sum(grad_out)[None]
    grad_attended = jnp.einsum(
        "std,ed->ste", grad_middle_b, proj_out, preferred_element_type=jnp.float32
    )
    grad_attended = grad_attended.astype(jnp.bfloat16).reshape(seqs, rows, head)
    row_terms = jnp.einsum(
        "srd,srd->sr", grad_attended, attended, preferred_element_type=jnp.float32
    )

    def backward_step(state, key_block, key_start):
        grad_queries, grad_keys = state
        scores, allowed = block_scores(key_block, key_start)
        probs = jnp.where(allowed, jnp.exp(scores - log_total[..., None]), 0.0)
        grad_probs = jnp.einsum(
            "srd,skd->srk", grad_attended, key_block[..., head:], preferred_element_type=jnp.float32
        )
        grad_scores = (probs * (grad_probs - row_terms[..., None])).astype(jnp.bfloat16)
        grad_queries = (
            grad_queries
            + jnp.einsum(
                "srk,skd->srd",
                grad_scores,
                key_block[..., :head],
                preferred_element_type=jnp.float32,
            )
            * SCALE
        )
        grad_key = (
            jnp.einsum("srk,srd->skd", grad_scores, queries, preferred_element_type=jnp.float32)
            * SCALE
        )
        grad_value = jnp.einsum(
            "srk,srd->skd",
            probs.astype(jnp.bfloat16),
            grad_attended,
            preferred_element_type=jnp.float32,
        )
        current = lax.dynamic_slice_in_dim(grad_keys, key_start, key_block.shape[1], 1)
        grad_keys = lax.dynamic_update_slice_in_dim(
            grad_keys, current + jnp.concatenate([grad_key, grad_value], axis=-1), key_start, 1
        )
        return (grad_queries, grad_keys)

    back_state = (
        jnp.zeros((seqs, rows, head), jnp.float32),
        jnp.zeros((seqs, seq_tokens, 2 * head), jnp.float32),
    )
    grad_queries, grad_keys = over_blocks(
        backward_step, back_state, gathered
    )
    grad_pairs = lax.dynamic_slice_in_dim(grad_keys, first_token, tokens, 1)
    for shift in range(1, n_ctx):
        place = (lax.axis_index("ctx") - shift) % n_ctx * tokens
        sent = to_bf16(lax.dynamic_slice_in_dim(grad_keys, place, tokens, 1))
        grad_pairs = grad_pairs + later(sent, shift).astype(jnp.float32)
    grad_q = unrotate(
        grad_queries.reshape(seqs, tokens, group, head), cosine[:, :, None, :], sine[:, :, None, :]
    )
    grad_k = unrotate(grad_pairs[..., :head], cosine, sine)
    grad_joined = jnp.concatenate(
        [grad_q.reshape(seqs, tokens, heads_width), grad_k, grad_pairs[..., head:]], axis=-1
    )
    grad_bias = jnp.sum(grad_joined, axis=(0, 1))[None]
    grad_joined_b = grad_joined.astype(jnp.bfloat16)
    joined_both = both_cores(grad_joined_b.reshape(flat, -1))
    grad_qkv = quarter_grads(
        lambda cols: jnp.einsum("td,te->de", cols, joined_both, preferred_element_type=jnp.float32),
        hidden_one.reshape(flat, -1),
    )
    grad_qkv = line_sum(grad_qkv)[:, None, :]
    back_mine = jnp.einsum(
        "ste,de->std", grad_joined_b, proj_qkv, preferred_element_type=jnp.float32
    )
    back_other = jnp.einsum(
        "ste,de->std", tp_other(grad_joined_b), other_qkv, preferred_element_type=jnp.float32
    )
    back_one = back_mine + back_other
    grad_gain_attn = jnp.sum(back_one * normed_one, axis=(0, 1))
    grad_input = grad_middle + norm_back(back_one, normed_one, scale_one, gain_attn)
    small = lax.psum((grad_gain_attn, grad_bias[0], grad_gain_mlp), ("dp", "ctx"))
    n_dp = lax.axis_size("dp")
    small = [
        lax.dynamic_slice_in_dim(v, lax.axis_index("dp") * (v.shape[0] // n_dp), v.shape[0] // n_dp)
        for v in small
    ]
    return (
        output,
        grad_input,
        small[0],
        grad_qkv,
        small[1][None],
        grad_out,
        small[2],
        grad_gate,
        grad_up,
        grad_down,
    )


def solution(mesh):
    in_specs = (
        P("dp", "ctx", None),
        P("dp", "ctx"),
        P(),
        P(None, "tp", None),
        P("tp", None),
        P("tp", None, None),
        P(),
        P(None, "tp"),
        P(None, "tp"),
        P("tp", None),
        P("dp", "ctx", None),
    )
    out_specs = (
        P("dp", "ctx", None),
        P("dp", "ctx", None),
        P("dp"),
        P("dp", "tp", None),
        P("tp", "dp"),
        P("tp", None, "dp"),
        P("dp"),
        P("dp", "tp"),
        P("dp", "tp"),
        P("tp", "dp"),
    )
    return jax.shard_map(shards, mesh=mesh, in_specs=in_specs, out_specs=out_specs, check_vma=False)
```

```python
import jax
import jax.numpy as jnp
from jax import lax
from jax.experimental import pallas as pl
from jax.experimental.pallas import tpu as pltpu
from jax.sharding import PartitionSpec as P

EPS = 1e-06
THETA = 1000000.0
SCALE = 0.125
NEGATIVE = -1e30
HD=64
F32=jnp.float32
BF=jnp.bfloat16

def dot(a, b):
    return jnp.dot(a, b, preferred_element_type=jnp.float32)

def dot_nt(a, b):
    return lax.dot_general(a, b, (((1,), (1,)), ((), ())), preferred_element_type=jnp.float32)

def turn(rows, cosine, sine):
    half = rows.shape[0] // 2
    first, second = rows[:half], rows[half:]
    return jnp.concatenate([first * cosine - second * sine, second * cosine + first * sine], axis=0)

def turn_back(rows, cosine, sine):
    return turn(rows, cosine, -sine)

def project_kernel(x_ref, gain_ref, w_ref, b_ref, cos_ref, sin_ref, hidden_ref, q_ref, kv_ref):
    x = x_ref[0].astype(F32)
    scale = lax.rsqrt(jnp.mean(x * x, axis=-1, keepdims=True) + EPS)
    hidden = (x * scale * gain_ref[...]).astype(BF)
    hidden_ref[0] = hidden
    joined = dot(hidden, w_ref[...]) + b_ref[...]
    turned = joined.T
    cosine, sine = cos_ref[0], sin_ref[0]
    width = q_ref.shape[1]
    for start in range(0, width, HD):
        q_ref[0, start:start + HD, :] = (turn(turned[start:start + HD], cosine, sine) * SCALE).astype(BF)
    keys = turn(turned[width:width + HD], cosine, sine)
    pair = jnp.concatenate([keys, turned[width + HD:]], axis=0)
    kv_ref[0] = pair.T.astype(BF)

def project(x, gain, w, b, cosine, sine, width):
    seqs, tokens, model = x.shape
    half = cosine.shape[1]
    whole = lambda a: pl.BlockSpec(a.shape, lambda s: (0,) * a.ndim)
    per = lambda r, c: pl.BlockSpec((1, r, c), lambda s: (s, 0, 0))
    return pl.pallas_call(
        project_kernel, grid=(seqs,),
        in_specs=[per(tokens, model), whole(gain), whole(w), whole(b), per(half, tokens), per(half, tokens)],
        out_specs=[per(tokens, model), per(width, tokens), per(tokens, 2 * HD)],
        out_shape=[jax.ShapeDtypeStruct((seqs, tokens, model), BF), jax.ShapeDtypeStruct((seqs, width, tokens), BF),
                   jax.ShapeDtypeStruct((seqs, tokens, 2 * HD), BF)],
        cost_estimate=pl.CostEstimate(flops=2 * seqs * tokens * model * w.shape[1], transcendentals=0, bytes_accessed=8 * seqs * tokens * model),
        name="project")(x, gain, w, b, cosine, sine)

def allowed_of(first_ref, place, s, tokens):
    key = lax.broadcasted_iota(jnp.int32, (tokens, tokens), 0) + (place - s * tokens)
    query = lax.broadcasted_iota(jnp.int32, (tokens, tokens), 1) + place
    return (key <= query) & (key >= first_ref[0])

def attend_kernel(info_ref, q_ref, kv_ref, first_ref, out_ref, lse_ref, top_ref, total_ref, acc_ref):
    seq = pl.program_id(0)
    tokens = q_ref.shape[2]
    heads = q_ref.shape[1] // HD
    place = info_ref[0]
    count, last_first = info_ref[1 + 2 * seq], info_ref[2 + 2 * seq]
    top_ref[...] = jnp.full_like(top_ref, NEGATIVE)
    total_ref[...] = jnp.zeros_like(total_ref)
    acc_ref[...] = jnp.zeros_like(acc_ref)

    def block(s, masked):
        pair = kv_ref[s, 0]
        keys = pair[:, :HD]
        values = pair.T[HD:]
        ok = allowed_of(first_ref, place, s, tokens) if masked else None
        for h in range(heads):
            rows = slice(h * HD, (h + 1) * HD)
            scores = dot(keys, q_ref[0, rows, :])
            if masked:
                scores = jnp.where(ok, scores, NEGATIVE)
            old = top_ref[h:h + 1, :]
            new = jnp.maximum(old, jnp.max(scores, axis=0, keepdims=True))
            weights = jnp.exp(scores - new)
            factor = jnp.exp(old - new)
            top_ref[h:h + 1, :] = new
            total_ref[h:h + 1, :] = total_ref[h:h + 1, :] * factor + jnp.sum(weights, axis=0, keepdims=True)
            acc_ref[rows, :] = acc_ref[rows, :] * factor + dot(values, weights.astype(BF))

    block(0, True)

    @pl.loop(1, count)
    def _(s):
        masked = last_first > place - s * tokens

        @pl.when(masked)
        def _():
            block(s, True)

        @pl.when(jnp.logical_not(masked))
        def _():
            block(s, False)

    lse_ref[0] = top_ref[...] + jnp.log(total_ref[...])
    for h in range(heads):
        rows = slice(h * HD, (h + 1) * HD)
        acc_ref[rows, :] = acc_ref[rows, :] / total_ref[h:h + 1, :]
    out_ref[0] = acc_ref[...].T.astype(BF)

def attend(info, q, kv, first):
    seqs, width, tokens = q.shape
    n = kv.shape[0]
    heads = width // HD
    pad = -(-heads // 8) * 8
    per = lambda r, c: pl.BlockSpec((1, r, c), lambda s, i: (s, 0, 0))
    return pl.pallas_call(
        attend_kernel,
        grid_spec=pltpu.PrefetchScalarGridSpec(
            num_scalar_prefetch=1, grid=(seqs,),
            in_specs=[per(width, tokens), pl.BlockSpec((n, 1, tokens, 2 * HD), lambda s, i: (0, s, 0, 0)), per(1, tokens)],
            out_specs=[per(tokens, width), per(pad, tokens)],
            scratch_shapes=[pltpu.VMEM((pad, tokens), F32), pltpu.VMEM((pad, tokens), F32), pltpu.VMEM((width, tokens), F32)]),
        out_shape=[jax.ShapeDtypeStruct((seqs, tokens, width), BF), jax.ShapeDtypeStruct((seqs, pad, tokens), F32)],
        cost_estimate=pl.CostEstimate(flops=8 * seqs * tokens * tokens * width * 2, transcendentals=seqs * heads * tokens * tokens * 2, bytes_accessed=8 * seqs * tokens * width),
        name="attend")(info, q, kv, first)

def attend_back_kernel(info_ref, grad_ref, w_ref, att_ref, q_ref, kv_ref, lse_ref, first_ref, cos_ref, sin_ref,
                       gq_ref, own_ref, sent_ref, bias_ref, gt_ref, qn_ref, gn_ref, term_ref, gacc_ref):
    seq = pl.program_id(0)
    tokens = q_ref.shape[2]
    heads = q_ref.shape[1] // HD
    place = info_ref[0]
    count, last_first = info_ref[1 + 2 * seq], info_ref[2 + 2 * seq]
    gt_ref[...] = dot_nt(w_ref[...], grad_ref[0]).astype(BF)
    att = att_ref[0].astype(F32).T
    for h in range(heads):
        rows = slice(h * HD, (h + 1) * HD)
        grad = gt_ref[rows, :].astype(F32)
        term_ref[h:h + 1, :] = jnp.sum(grad * att[rows], axis=0, keepdims=True)
        gn_ref[h] = grad.T.astype(BF)
        qn_ref[h] = q_ref[0, rows, :].astype(F32).T.astype(BF)
    gacc_ref[...] = jnp.zeros_like(gacc_ref)

    def block(s, masked):
        pair = kv_ref[s, 0]
        keys, values = pair[:, :HD], pair[:, HD:]
        keys_t = pair.T[:HD]
        ok = allowed_of(first_ref, place, s, tokens) if masked else None
        grad_key = jnp.zeros((tokens, HD), F32)
        grad_value = jnp.zeros((tokens, HD), F32)
        for h in range(heads):
            rows = slice(h * HD, (h + 1) * HD)
            scores = dot(keys, q_ref[0, rows, :])
            probs = jnp.exp(scores - lse_ref[0, h:h + 1, :])
            if masked:
                probs = jnp.where(ok, probs, 0.0)
            grad_probs = dot(values, gt_ref[rows, :])
            grad_scores = (probs * (grad_probs - term_ref[h:h + 1, :])).astype(BF)
            grad_value = grad_value + dot(probs.astype(BF), gn_ref[h])
            grad_key = grad_key + dot(grad_scores, qn_ref[h])
            gacc_ref[rows, :] = gacc_ref[rows, :] + dot(keys_t, grad_scores)
        return jnp.concatenate([grad_key, grad_value], axis=1)

    own_ref[0] = block(0, True)

    @pl.loop(1, sent_ref.shape[0] + 1)
    def _(s):
        masked = last_first > place - s * tokens

        @pl.when(s >= count)
        def _():
            sent_ref[s - 1, 0] = jnp.zeros((tokens, 2 * HD), BF)

        @pl.when((s < count) & masked)
        def _():
            sent_ref[s - 1, 0] = block(s, True).astype(BF)

        @pl.when((s < count) & jnp.logical_not(masked))
        def _():
            sent_ref[s - 1, 0] = block(s, False).astype(BF)

    cosine, sine = cos_ref[0], sin_ref[0]
    for h in range(heads):
        rows = slice(h * HD, (h + 1) * HD)
        gacc_ref[rows, :] = turn_back(gacc_ref[rows, :] * SCALE, cosine, sine)
    out = gacc_ref[...].T
    gq_ref[0] = out.astype(BF)
    bias_ref[0] = jnp.sum(out, axis=0, keepdims=True)

def attend_back(info, grad, w, att, q, kv, lse, first, cosine, sine):
    seqs, width, tokens = q.shape
    model = grad.shape[-1]
    n = kv.shape[0]
    heads = width // HD
    pad = lse.shape[1]
    half = cosine.shape[1]
    per = lambda r, c: pl.BlockSpec((1, r, c), lambda s, i: (s, 0, 0))
    blocks = lambda k: pl.BlockSpec((k, 1, tokens, 2 * HD), lambda s, i: (0, s, 0, 0))
    return pl.pallas_call(
        attend_back_kernel,
        grid_spec=pltpu.PrefetchScalarGridSpec(
            num_scalar_prefetch=1, grid=(seqs,),
            in_specs=[per(tokens, model), pl.BlockSpec(w.shape, lambda s, i: (0, 0)), per(tokens, width), per(width, tokens),
                      blocks(n), per(pad, tokens), per(1, tokens), per(half, tokens), per(half, tokens)],
            out_specs=[per(tokens, width), per(tokens, 2 * HD), blocks(n - 1), per(1, width)],
            scratch_shapes=[pltpu.VMEM((width, tokens), BF), pltpu.VMEM((heads, tokens, HD), BF), pltpu.VMEM((heads, tokens, HD), BF),
                            pltpu.VMEM((pad, tokens), F32), pltpu.VMEM((width, tokens), F32)]),
        out_shape=[jax.ShapeDtypeStruct((seqs, tokens, width), BF), jax.ShapeDtypeStruct((seqs, tokens, 2 * HD), F32),
                   jax.ShapeDtypeStruct((n - 1, seqs, tokens, 2 * HD), BF), jax.ShapeDtypeStruct((seqs, 1, width), F32)],
        cost_estimate=pl.CostEstimate(flops=20 * seqs * tokens * tokens * width * 2, transcendentals=seqs * heads * tokens * tokens * 2, bytes_accessed=16 * seqs * tokens * width),
        name="attend_back")(info, grad, w, att, q, kv, lse, first, cosine, sine)


def to_bf16(values):
    return values.astype(jnp.bfloat16)


def tp_other(values):
    return lax.ppermute(values, "tp", [(0, 1), (1, 0)])


def tp_sum(values):
    mine = to_bf16(values)
    return mine.astype(jnp.float32) + tp_other(mine).astype(jnp.float32)


def core_other(values):
    pairs = [(i, i ^ 1) for i in range(lax.axis_size("dp"))]
    return lax.ppermute(values, "dp", pairs)


def earlier(values, shift):
    n = lax.axis_size("ctx")
    return lax.ppermute(values, "ctx", [(i, i + shift) for i in range(n - shift)])


def later(values, shift):
    n = lax.axis_size("ctx")
    return lax.ppermute(values, "ctx", [(i + shift, i) for i in range(n - shift)])


def line_sum(part):
    n = lax.axis_size("ctx")
    half = n // 2
    me = lax.axis_index("ctx")
    for step in range(half - 1):
        pairs = [(step, step + 1), (n - 1 - step, n - 2 - step)]
        part = part + lax.ppermute(to_bf16(part), "ctx", pairs).astype(jnp.float32)
    mine = to_bf16(part)
    moved = lax.ppermute(mine, "ctx", [(half - 1, half), (half, half - 1)])
    total = to_bf16(mine.astype(jnp.float32) + moved.astype(jnp.float32))
    for step in reversed(range(half - 1)):
        pairs = [(step + 1, step), (n - 2 - step, n - 1 - step)]
        moved = lax.ppermute(total, "ctx", pairs)
        total = jnp.where((me == step) | (me == n - 1 - step), moved, total)
    return total.astype(jnp.float32)


def quarter_grads(make, wide):
    n_dp = lax.axis_size("dp")
    rows = n_dp // 2
    me = lax.axis_index("dp")
    row, core = me // 2, me % 2
    split = wide.reshape(wide.shape[0], rows, 2, wide.shape[1] // n_dp)
    mine = lax.dynamic_index_in_dim(split, core, 2, keepdims=False)
    theirs = core_other(lax.dynamic_index_in_dim(split, 1 - core, 2, keepdims=False))
    both = jnp.concatenate([mine, theirs], axis=0)

    def columns(which):
        return lax.dynamic_index_in_dim(both, which, 1, keepdims=False)

    total = None
    for shift in range(1, rows):
        part = to_bf16(make(columns((row + shift) % rows)))
        pairs = [(r * 2 + c, ((r + shift) % rows) * 2 + c) for r in range(rows) for c in range(2)]
        moved = lax.ppermute(part, "dp", pairs).astype(jnp.float32)
        total = moved if total is None else total + moved
    own = make(columns(row))
    return own if total is None else own + total


def both_cores(values):
    return jnp.concatenate([values, core_other(values)], axis=0)


def inverse_rms(values):
    return lax.rsqrt(jnp.mean(values * values, axis=-1, keepdims=True) + EPS)


def norm_back(grad_h, normed, scale, gain):
    upstream = grad_h * gain
    inner = jnp.mean(upstream * normed, axis=-1, keepdims=True)
    return scale * (upstream - normed * inner)


def shards(
    block_input,
    positions,
    gain_attn,
    w_qkv,
    b_qkv,
    w_out,
    gain_mlp,
    w_gate,
    w_up,
    w_down,
    cotangent,
):
    seqs, tokens, _ = block_input.shape
    flat = seqs * tokens
    heads_width = w_out.shape[1]
    n_ctx = lax.axis_size("ctx")
    me = lax.axis_index("ctx")
    first_token = me * tokens
    proj_qkv = w_qkv[:, 0, :]
    proj_out = w_out[0]
    other_qkv = tp_other(proj_qkv)
    other_out = tp_other(proj_out)
    half = HD // 2
    freq = THETA ** (-(jnp.arange(half, dtype=jnp.float32) * 2.0) / HD)
    angle = positions.astype(jnp.float32)[:, None, :] * freq[None, :, None]
    cosine, sine = jnp.cos(angle), jnp.sin(angle)
    token_index = first_token + jnp.arange(tokens, dtype=jnp.int32)
    query_first = token_index[None, :] - positions
    counts = me - query_first[:, 0] // tokens + 1
    info = jnp.concatenate(
        [first_token[None], jnp.stack([counts, query_first[:, -1]], axis=1).reshape(-1)]
    ).astype(jnp.int32)
    query_first = query_first[:, None, :]

    hidden_one, queries, key_value = project(
        block_input, gain_attn[None, :], proj_qkv, b_qkv, cosine, sine, heads_width
    )
    pairs = jnp.stack([key_value] + [earlier(key_value, shift) for shift in range(1, n_ctx)])
    grad_act = jnp.einsum("std,fd->stf", cotangent, w_down, preferred_element_type=jnp.float32)
    attended, lse = attend(info, queries, pairs, query_first)
    inputs = block_input.astype(jnp.float32)
    attn_mine = jnp.einsum(
        "ste,ed->std", attended, proj_out, preferred_element_type=jnp.float32
    )
    attn_other = jnp.einsum(
        "ste,ed->std", tp_other(attended), other_out, preferred_element_type=jnp.float32
    )
    middle = inputs + (attn_mine + attn_other)
    scale_two = inverse_rms(middle)
    normed_two = middle * scale_two
    hidden_two = (normed_two * gain_mlp).astype(jnp.bfloat16)
    gate = jnp.einsum("std,df->stf", hidden_two, w_gate, preferred_element_type=jnp.float32)
    up = jnp.einsum("std,df->stf", hidden_two, w_up, preferred_element_type=jnp.float32)
    sigma = jax.nn.sigmoid(gate)
    activated = (gate * sigma * up).astype(jnp.bfloat16)
    mlp_part = jnp.einsum("stf,fd->std", activated, w_down, preferred_element_type=jnp.float32)
    output = (middle + tp_sum(mlp_part)).astype(jnp.bfloat16)
    grad_gate_in = (grad_act * up * sigma * (1.0 + gate * (1.0 - sigma))).astype(jnp.bfloat16)
    grad_up_in = (grad_act * gate * sigma).astype(jnp.bfloat16)
    acts = both_cores(activated.reshape(flat, -1))
    gates = both_cores(grad_gate_in.reshape(flat, -1))
    ups = both_cores(grad_up_in.reshape(flat, -1))
    grad_down = quarter_grads(
        lambda cols: jnp.einsum("tf,td->fd", acts, cols, preferred_element_type=jnp.float32),
        cotangent.reshape(flat, -1),
    )
    hidden_flat = hidden_two.reshape(flat, -1)
    grad_gate = quarter_grads(
        lambda cols: jnp.einsum("td,tf->df", cols, gates, preferred_element_type=jnp.float32),
        hidden_flat,
    )
    grad_up = quarter_grads(
        lambda cols: jnp.einsum("td,tf->df", cols, ups, preferred_element_type=jnp.float32),
        hidden_flat,
    )
    grad_down = line_sum(grad_down)
    grad_gate = line_sum(grad_gate)
    grad_up = line_sum(grad_up)
    back_two = jnp.einsum("stf,df->std", grad_gate_in, w_gate, preferred_element_type=jnp.float32)
    back_two = back_two + jnp.einsum(
        "stf,df->std", grad_up_in, w_up, preferred_element_type=jnp.float32
    )
    back_two = tp_sum(back_two)
    grad_gain_mlp = jnp.sum(back_two * normed_two, axis=(0, 1))
    grad_middle = cotangent.astype(jnp.float32) + norm_back(
        back_two, normed_two, scale_two, gain_mlp
    )
    grad_middle_b = grad_middle.astype(jnp.bfloat16)
    att_both = both_cores(attended.reshape(flat, -1))
    grad_out = quarter_grads(
        lambda cols: jnp.einsum("te,td->ed", att_both, cols, preferred_element_type=jnp.float32),
        grad_middle_b.reshape(flat, -1),
    )
    grad_out = line_sum(grad_out)[None]

    grad_q, grad_own, grad_sent, bias_q = attend_back(
        info, grad_middle_b, proj_out, attended, queries, pairs, lse, query_first, cosine, sine
    )
    grad_pairs = grad_own
    for shift in range(1, n_ctx):
        grad_pairs = grad_pairs + later(grad_sent[shift - 1], shift).astype(jnp.float32)
    cos_rows, sin_rows = jnp.swapaxes(cosine, 1, 2), jnp.swapaxes(sine, 1, 2)
    one, two = grad_pairs[..., :half], grad_pairs[..., half:HD]
    grad_kv = jnp.concatenate(
        [one * cos_rows + two * sin_rows, two * cos_rows - one * sin_rows, grad_pairs[..., HD:]],
        axis=-1,
    )
    grad_bias = jnp.concatenate([jnp.sum(bias_q, axis=(0, 1)), jnp.sum(grad_kv, axis=(0, 1))])
    grad_joined_b = jnp.concatenate([grad_q, to_bf16(grad_kv)], axis=-1)
    joined_both = both_cores(grad_joined_b.reshape(flat, -1))
    grad_qkv = quarter_grads(
        lambda cols: jnp.einsum("td,te->de", cols, joined_both, preferred_element_type=jnp.float32),
        hidden_one.reshape(flat, -1),
    )
    grad_qkv = line_sum(grad_qkv)[:, None, :]
    back_mine = jnp.einsum(
        "ste,de->std", grad_joined_b, proj_qkv, preferred_element_type=jnp.float32
    )
    back_other = jnp.einsum(
        "ste,de->std", tp_other(grad_joined_b), other_qkv, preferred_element_type=jnp.float32
    )
    back_one = back_mine + back_other
    scale_one = inverse_rms(inputs)
    normed_one = inputs * scale_one
    grad_gain_attn = jnp.sum(back_one * normed_one, axis=(0, 1))
    grad_input = grad_middle + norm_back(back_one, normed_one, scale_one, gain_attn)
    small = lax.psum((grad_gain_attn, grad_bias, grad_gain_mlp), ("dp", "ctx"))
    n_dp = lax.axis_size("dp")
    small = [
        lax.dynamic_slice_in_dim(v, lax.axis_index("dp") * (v.shape[0] // n_dp), v.shape[0] // n_dp)
        for v in small
    ]
    return (
        output,
        grad_input,
        small[0],
        grad_qkv,
        small[1][None],
        grad_out,
        small[2],
        grad_gate,
        grad_up,
        grad_down,
    )


def solution(mesh):
    in_specs = (
        P("dp", "ctx", None),
        P("dp", "ctx"),
        P(),
        P(None, "tp", None),
        P("tp", None),
        P("tp", None, None),
        P(),
        P(None, "tp"),
        P(None, "tp"),
        P("tp", None),
        P("dp", "ctx", None),
    )
    out_specs = (
        P("dp", "ctx", None),
        P("dp", "ctx", None),
        P("dp"),
        P("dp", "tp", None),
        P("tp", "dp"),
        P("tp", None, "dp"),
        P("dp"),
        P("dp", "tp"),
        P("dp", "tp"),
        P("tp", "dp"),
    )
    return jax.shard_map(shards, mesh=mesh, in_specs=in_specs, out_specs=out_specs, check_vma=False)
```

```python
import functools

import jax
import jax.numpy as jnp
from jax import lax
from jax.experimental import pallas as pl
from jax.experimental.pallas import tpu as pltpu
from jax.sharding import PartitionSpec as P

EPS = 1e-06
THETA = 1000000.0
SCALE = 0.125
NEGATIVE = -1e30
HD = 64
F32 = jnp.float32
BF = jnp.bfloat16
VMEM_LIMIT = 60 * 2**20


def shape_of(shape, dtype):
    return jax.ShapeDtypeStruct(shape, dtype)


def dot(a, b):
    return jnp.dot(a, b, preferred_element_type=F32)


def dot_nt(a, b):
    return lax.dot_general(a, b, (((1,), (1,)), ((), ())), preferred_element_type=F32)


def turn(rows, cosine, sine):
    half = rows.shape[0] // 2
    first, second = rows[:half], rows[half:]
    return jnp.concatenate([first * cosine - second * sine, second * cosine + first * sine], axis=0)


def inverse_rms(values):
    return lax.rsqrt(jnp.mean(values * values, axis=-1, keepdims=True) + EPS)


def norm_back(back, normed, scale, gain):
    upstream = back * gain
    inner = jnp.mean(upstream * normed, axis=-1, keepdims=True)
    return scale * (upstream - normed * inner)


def whole(a):
    return pl.BlockSpec(a.shape, lambda *_: (0,) * a.ndim)


def row_of(a, seq):
    return pl.BlockSpec((1,) + a.shape[1:], lambda *_: (seq,) + (0,) * (a.ndim - 1))


def full(*shape):
    return pl.BlockSpec(shape, lambda *_: (0,) * len(shape))


def params():
    return pltpu.CompilerParams(vmem_limit_bytes=VMEM_LIMIT)


def project_kernel(x_ref, gain_ref, w_ref, b_ref, cos_ref, sin_ref, hidden_ref, q_ref, kv_ref):
    x = x_ref[0].astype(F32)
    hidden = x * inverse_rms(x) * gain_ref[...]
    hidden_ref[0] = hidden.T.astype(BF)
    turned = (dot(hidden.astype(BF), w_ref[...]) + b_ref[...]).T
    cosine, sine = cos_ref[0], sin_ref[0]
    width = q_ref.shape[1]
    for start in range(0, width, HD):
        rows = slice(start, start + HD)
        q_ref[0, rows, :] = (turn(turned[rows], cosine, sine) * SCALE).astype(BF)
    keys = turn(turned[width : width + HD], cosine, sine)
    kv_ref[0] = jnp.concatenate([keys, turned[width + HD :]], axis=0).T.astype(BF)


def project(x, gain, w, b, cosine, sine, width):
    seqs, tokens, model = x.shape
    per = lambda r, c: pl.BlockSpec((1, r, c), lambda s: (s, 0, 0))
    half = cosine.shape[1]
    return pl.pallas_call(
        project_kernel,
        grid=(seqs,),
        in_specs=[
            per(tokens, model),
            whole(gain),
            whole(w),
            whole(b),
            per(half, tokens),
            per(half, tokens),
        ],
        out_specs=[per(model, tokens), per(width, tokens), per(tokens, 2 * HD)],
        out_shape=[
            shape_of((seqs, model, tokens), BF),
            shape_of((seqs, width, tokens), BF),
            shape_of((seqs, tokens, 2 * HD), BF),
        ],
        cost_estimate=pl.CostEstimate(
            flops=2 * seqs * tokens * model * w.shape[1],
            transcendentals=0,
            bytes_accessed=8 * seqs * tokens * model,
        ),
        compiler_params=params(),
        name="project",
    )(x, gain, w, b, cosine, sine)


def allowed_of(first_ref, place, back, tokens):
    shape = (tokens, tokens)
    key = lax.broadcasted_iota(jnp.int32, shape, 0) + (place - back * tokens)
    query = lax.broadcasted_iota(jnp.int32, shape, 1) + place
    return (key <= query) & (key >= first_ref[0])


def attend_kernel(n, seq, info_ref, q_ref, first_ref, *refs):
    pair_refs, (out_ref, lse_ref, pairs_ref, top_ref, total_ref, acc_ref) = refs[:n], refs[n:]
    tokens = q_ref.shape[2]
    heads = q_ref.shape[1] // HD
    place = info_ref[0]
    count, last_first = info_ref[1 + 2 * seq], info_ref[2 + 2 * seq]
    for s in range(n):
        pairs_ref[s] = pair_refs[s][0]
    top_ref[...] = jnp.full_like(top_ref, NEGATIVE)
    total_ref[...] = jnp.zeros_like(total_ref)
    acc_ref[...] = jnp.zeros_like(acc_ref)

    def block(back, masked):
        pair = pairs_ref[back]
        keys = pair[:, :HD]
        values = pair.T[HD:]
        ok = allowed_of(first_ref, place, back, tokens) if masked else None
        for h in range(heads):
            rows = slice(h * HD, (h + 1) * HD)
            scores = dot(keys, q_ref[0, rows, :])
            if masked:
                scores = jnp.where(ok, scores, NEGATIVE)
            old = top_ref[h : h + 1, :]
            new = jnp.maximum(old, jnp.max(scores, axis=0, keepdims=True))
            weights = jnp.exp(scores - new)
            factor = jnp.exp(old - new)
            top_ref[h : h + 1, :] = new
            total_ref[h : h + 1, :] = total_ref[h : h + 1, :] * factor + jnp.sum(
                weights, axis=0, keepdims=True
            )
            acc_ref[rows, :] = acc_ref[rows, :] * factor + dot(values, weights.astype(BF))

    block(0, True)

    @pl.loop(1, count)
    def _(back):
        masked = last_first > place - back * tokens

        @pl.when(masked)
        def _():
            block(back, True)

        @pl.when(jnp.logical_not(masked))
        def _():
            block(back, False)

    lse_ref[...] = top_ref[...] + jnp.log(total_ref[...])
    for h in range(heads):
        rows = slice(h * HD, (h + 1) * HD)
        acc_ref[rows, :] = acc_ref[rows, :] / total_ref[h : h + 1, :]
    out_ref[...] = acc_ref[...].T.astype(BF)


def attend(seq, info, q, pairs, first):
    _, width, tokens = q.shape
    n = len(pairs)
    heads = width // HD
    pad = -(-heads // 8) * 8
    return pl.pallas_call(
        functools.partial(attend_kernel, n, seq),
        grid_spec=pltpu.PrefetchScalarGridSpec(
            num_scalar_prefetch=1,
            grid=(1,),
            in_specs=[row_of(q, seq), row_of(first, seq)] + [row_of(p, seq) for p in pairs],
            out_specs=[full(tokens, width), full(pad, tokens)],
            scratch_shapes=[
                pltpu.VMEM((n, tokens, 2 * HD), BF),
                pltpu.VMEM((pad, tokens), F32),
                pltpu.VMEM((pad, tokens), F32),
                pltpu.VMEM((width, tokens), F32),
            ],
        ),
        out_shape=[shape_of((tokens, width), BF), shape_of((pad, tokens), F32)],
        cost_estimate=pl.CostEstimate(
            flops=8 * tokens * tokens * width,
            transcendentals=2 * heads * tokens * tokens,
            bytes_accessed=16 * tokens * width,
        ),
        compiler_params=params(),
        name="attend",
    )(info, q, first, *pairs)


def attend_back_kernel(
    n,
    seq,
    info_ref,
    mine_ref,
    other_ref,
    middle_ref,
    cot_ref,
    gain_ref,
    w_ref,
    att_ref,
    q_ref,
    lse_ref,
    first_ref,
    cos_ref,
    sin_ref,
    *refs,
):
    pair_refs, refs = refs[:n], refs[n:]
    gmid_ref, gmid_t_ref, gain_out_ref, gq_ref, bias_ref, own_ref = refs[:6]
    sent_refs, refs = refs[6 : 6 + n - 1], refs[6 + n - 1 :]
    pairs_ref, sent_ref, gt_ref, qn_ref, gn_ref, term_ref, gacc_ref = refs
    tokens = q_ref.shape[2]
    heads = q_ref.shape[1] // HD
    place = info_ref[0]
    count, last_first = info_ref[1 + 2 * seq], info_ref[2 + 2 * seq]
    for s in range(n):
        pairs_ref[s] = pair_refs[s][0]

    middle = middle_ref[...]
    scale = inverse_rms(middle)
    normed = middle * scale
    back = mine_ref[...].astype(F32) + other_ref[...].astype(F32)
    gain_out_ref[...] = jnp.sum(back * normed, axis=0, keepdims=True)
    gmid = cot_ref[0].astype(F32) + norm_back(back, normed, scale, gain_ref[...])
    gmid_ref[...] = gmid
    gmid_t = gmid.T.astype(BF)
    gmid_t_ref[...] = gmid_t
    gt_ref[...] = dot(w_ref[...], gmid_t).astype(BF)
    att = att_ref[...].astype(F32).T
    for h in range(heads):
        rows = slice(h * HD, (h + 1) * HD)
        grad = gt_ref[rows, :].astype(F32)
        term_ref[h : h + 1, :] = jnp.sum(grad * att[rows], axis=0, keepdims=True)
        gn_ref[h] = grad.T.astype(BF)
        qn_ref[h] = q_ref[0, rows, :].astype(F32).T.astype(BF)
    gacc_ref[...] = jnp.zeros_like(gacc_ref)

    def block(back, masked):
        pair = pairs_ref[back]
        keys, values = pair[:, :HD], pair[:, HD:]
        keys_t = pair.T[:HD]
        ok = allowed_of(first_ref, place, back, tokens) if masked else None
        grad_key = jnp.zeros((tokens, HD), F32)
        grad_value = jnp.zeros((tokens, HD), F32)
        for h in range(heads):
            rows = slice(h * HD, (h + 1) * HD)
            scores = dot(keys, q_ref[0, rows, :])
            probs = jnp.exp(scores - lse_ref[h : h + 1, :])
            if masked:
                probs = jnp.where(ok, probs, 0.0)
            grad_probs = dot(values, gt_ref[rows, :])
            grad_scores = (probs * (grad_probs - term_ref[h : h + 1, :])).astype(BF)
            grad_value = grad_value + dot(probs.astype(BF), gn_ref[h])
            grad_key = grad_key + dot(grad_scores, qn_ref[h])
            gacc_ref[rows, :] = gacc_ref[rows, :] + dot(keys_t, grad_scores)
        return jnp.concatenate([grad_key, grad_value], axis=1)

    own_ref[...] = block(0, True)

    @pl.loop(1, n)
    def _(back):
        masked = last_first > place - back * tokens

        @pl.when(back >= count)
        def _():
            sent_ref[back - 1] = jnp.zeros((tokens, 2 * HD), BF)

        @pl.when((back < count) & masked)
        def _():
            sent_ref[back - 1] = block(back, True).astype(BF)

        @pl.when((back < count) & jnp.logical_not(masked))
        def _():
            sent_ref[back - 1] = block(back, False).astype(BF)

    for s in range(n - 1):
        sent_refs[s][...] = sent_ref[s]
    cosine, sine = cos_ref[0], sin_ref[0]
    for h in range(heads):
        rows = slice(h * HD, (h + 1) * HD)
        gacc_ref[rows, :] = turn(gacc_ref[rows, :] * SCALE, cosine, -sine)
    out = gacc_ref[...].T
    gq_ref[...] = out.astype(BF)
    bias_ref[...] = jnp.sum(out, axis=0, keepdims=True)


def attend_back(seq, info, mine, other, middle, cot, gain, w, att, q, lse, first, cosine, sine, pairs):
    _, width, tokens = q.shape
    model = w.shape[1]
    n = len(pairs)
    heads = width // HD
    pad = lse.shape[0]
    pair = (tokens, 2 * HD)
    return pl.pallas_call(
        functools.partial(attend_back_kernel, n, seq),
        grid_spec=pltpu.PrefetchScalarGridSpec(
            num_scalar_prefetch=1,
            grid=(1,),
            in_specs=[
                whole(mine),
                whole(other),
                whole(middle),
                row_of(cot, seq),
                whole(gain),
                whole(w),
                whole(att),
                row_of(q, seq),
                whole(lse),
                row_of(first, seq),
                row_of(cosine, seq),
                row_of(sine, seq),
            ]
            + [row_of(p, seq) for p in pairs],
            out_specs=[
                full(tokens, model),
                full(model, tokens),
                full(1, model),
                full(tokens, width),
                full(1, width),
                full(*pair),
            ]
            + [full(*pair)] * (n - 1),
            scratch_shapes=[
                pltpu.VMEM((n,) + pair, BF),
                pltpu.VMEM((n - 1,) + pair, BF),
                pltpu.VMEM((width, tokens), BF),
                pltpu.VMEM((heads, tokens, HD), BF),
                pltpu.VMEM((heads, tokens, HD), BF),
                pltpu.VMEM((pad, tokens), F32),
                pltpu.VMEM((width, tokens), F32),
            ],
        ),
        out_shape=[
            shape_of((tokens, model), F32),
            shape_of((model, tokens), BF),
            shape_of((1, model), F32),
            shape_of((tokens, width), BF),
            shape_of((1, width), F32),
            shape_of(pair, F32),
        ]
        + [shape_of(pair, BF)] * (n - 1),
        cost_estimate=pl.CostEstimate(
            flops=24 * tokens * tokens * width,
            transcendentals=2 * heads * tokens * tokens,
            bytes_accessed=16 * tokens * model,
        ),
        compiler_params=params(),
        name="attend_back",
    )(info, mine, other, middle, cot, gain, w, att, q, lse, first, cosine, sine, *pairs)


def mlp_kernel(
    total,
    x_ref,
    mine_ref,
    other_ref,
    wo_ref,
    wx_ref,
    gain_ref,
    cot_ref,
    gate_ref,
    up_ref,
    down_ref,
    middle_ref,
    hid_t_ref,
    act_ref,
    gg_ref,
    gu_ref,
    part_ref,
    back_ref,
    hidden_ref,
    acc_ref,
    bacc_ref,
):
    j = pl.program_id(0)

    @pl.when(j == 0)
    def _():
        middle = x_ref[0].astype(F32) + (
            dot(mine_ref[...], wo_ref[...]) + dot(other_ref[...], wx_ref[...])
        )
        middle_ref[...] = middle
        hidden = middle * inverse_rms(middle) * gain_ref[...]
        hidden_ref[...] = hidden.astype(BF)
        hid_t_ref[...] = hidden.T.astype(BF)
        acc_ref[...] = jnp.zeros_like(acc_ref)
        bacc_ref[...] = jnp.zeros_like(bacc_ref)

    tile = gate_ref.shape[1]
    wg, wu, wd = gate_ref[...], up_ref[...], down_ref[...]
    if total % tile:
        left = total - j * tile
        cols = lax.broadcasted_iota(jnp.int32, wg.shape, 1) < left
        wg, wu = jnp.where(cols, wg, jnp.zeros_like(wg)), jnp.where(cols, wu, jnp.zeros_like(wu))
        rows = lax.broadcasted_iota(jnp.int32, wd.shape, 0) < left
        wd = jnp.where(rows, wd, jnp.zeros_like(wd))
    hidden = hidden_ref[...]
    gate = dot(hidden, wg)
    up = dot(hidden, wu)
    grad_act = dot_nt(cot_ref[0], wd)
    sigma = 1.0 / (1.0 + jnp.exp(-gate))
    silu = gate * sigma
    act = (silu * up).astype(BF)
    gg = (grad_act * up * sigma * (1.0 + gate * (1.0 - sigma))).astype(BF)
    gu = (grad_act * silu).astype(BF)
    act_ref[...] = act
    gg_ref[...] = gg
    gu_ref[...] = gu
    acc_ref[...] += dot(act, wd)
    bacc_ref[...] += dot_nt(gg, wg) + dot_nt(gu, wu)

    @pl.when(j == pl.num_programs(0) - 1)
    def _():
        part_ref[...] = acc_ref[...].astype(BF)
        back_ref[...] = bacc_ref[...].astype(BF)


def mlp(seq, x, mine, other, wo, wx, gain, cot, wg, wu, wd, tile=512):
    _, tokens, model = x.shape
    ff = wg.shape[1]
    cols = pl.BlockSpec((tokens, tile), lambda j: (0, j))
    columns = pl.BlockSpec((model, tile), lambda j: (0, j))
    return pl.pallas_call(
        functools.partial(mlp_kernel, ff),
        grid=(pl.cdiv(ff, tile),),
        in_specs=[
            row_of(x, seq),
            whole(mine),
            whole(other),
            whole(wo),
            whole(wx),
            whole(gain),
            row_of(cot, seq),
            columns,
            columns,
            pl.BlockSpec((tile, model), lambda j: (j, 0)),
        ],
        out_specs=[full(tokens, model), full(model, tokens)]
        + [cols] * 3
        + [full(tokens, model)] * 2,
        out_shape=[shape_of((tokens, model), F32), shape_of((model, tokens), BF)]
        + [shape_of((tokens, ff), BF)] * 3
        + [shape_of((tokens, model), BF)] * 2,
        scratch_shapes=[
            pltpu.VMEM((tokens, model), BF),
            pltpu.VMEM((tokens, model), F32),
            pltpu.VMEM((tokens, model), F32),
        ],
        cost_estimate=pl.CostEstimate(
            flops=12 * tokens * model * ff,
            transcendentals=tokens * ff,
            bytes_accessed=6 * model * ff + 6 * tokens * ff,
        ),
        compiler_params=params(),
        name="mlp",
    )(x, mine, other, wo, wx, gain, cot, wg, wu, wd)


def weight_kernel(count, shares, places_ref, *refs):
    lefts, rights, outs = refs[: 2 * count], refs[2 * count : 4 * count], refs[4 * count :]
    for share in range(shares):
        total = None
        for k in range(2 * count):
            place = places_ref[share if k < count else shares + share]
            part = dot(lefts[k][place], rights[k][...])
            total = part if total is None else total + part
        outs[share][...] = total.astype(outs[share].dtype)


def weight_grad(places, lefts, rights, tile):
    count = len(lefts) // 2
    shares = places.shape[0] // 2
    _, rows, tokens = lefts[0].shape
    ff = rights[0].shape[1]
    tile = min(tile, ff)
    cols = pl.BlockSpec((tokens, tile), lambda j, p: (0, j))
    out = pl.BlockSpec((rows, tile), lambda j, p: (0, j))
    return pl.pallas_call(
        functools.partial(weight_kernel, count, shares),
        grid_spec=pltpu.PrefetchScalarGridSpec(
            num_scalar_prefetch=1,
            grid=(pl.cdiv(ff, tile),),
            in_specs=[whole(a) for a in lefts] + [cols] * len(rights),
            out_specs=[out] * shares,
        ),
        out_shape=[shape_of((rows, ff), F32)] + [shape_of((rows, ff), BF)] * (shares - 1),
        cost_estimate=pl.CostEstimate(
            flops=4 * count * shares * rows * tokens * ff,
            transcendentals=0,
            bytes_accessed=4 * count * tokens * ff + 6 * rows * ff,
        ),
        compiler_params=params(),
        name="weight_grad",
    )(places, *lefts, *rights)


def pair_back_kernel(own_ref, cos_ref, sin_ref, *refs):
    moved, out_ref, bias_ref = refs[:-2], refs[-2], refs[-1]
    total = own_ref[...]
    for ref in moved:
        total = total + ref[...].astype(F32)
    turned = total.T
    keys = turn(turned[:HD], cos_ref[0], -sin_ref[0])
    total = jnp.concatenate([keys, turned[HD:]], axis=0).T
    out_ref[...] = total.astype(BF)
    bias_ref[...] = jnp.sum(total, axis=0, keepdims=True)


def pair_back(seq, own, moved, cosine, sine):
    return pl.pallas_call(
        pair_back_kernel,
        grid=(1,),
        in_specs=[whole(own), row_of(cosine, seq), row_of(sine, seq)] + [whole(m) for m in moved],
        out_specs=[full(*own.shape), full(1, own.shape[1])],
        out_shape=[shape_of(own.shape, BF), shape_of((1, own.shape[1]), F32)],
        compiler_params=params(),
        name="pair_back",
    )(own, cosine, sine, *moved)


def input_back_kernel(
    gq_ref, gqx_ref, gkv_ref, gkvx_ref, w_ref, wx_ref, x_ref, gain_ref, gmid_ref, *refs
):
    out_ref, gain_out_ref = refs[-2:]
    width = gq_ref.shape[1]

    def back_of(q_ref, kv_ref, weights):
        return dot_nt(q_ref[...], weights[:, :width]) + dot_nt(kv_ref[...], weights[:, width:])

    back = back_of(gq_ref, gkv_ref, w_ref[...]) + back_of(gqx_ref, gkvx_ref, wx_ref[...])
    x = x_ref[0].astype(F32)
    scale = inverse_rms(x)
    normed = x * scale
    gain_out_ref[...] = jnp.sum(back * normed, axis=0, keepdims=True)
    out_ref[0] = gmid_ref[...] + norm_back(back, normed, scale, gain_ref[...])


def input_back(seq, gq, gqx, gkv, gkvx, w, wx, x, gain, gmid, so_far):
    seqs, tokens, model = x.shape
    operands = [gq, gqx, gkv, gkvx, w, wx, x, gain, gmid]
    specs = [whole(a) for a in operands]
    specs[6] = row_of(x, seq)
    aliases = {}
    if so_far is not None:
        aliases = {len(operands): 0}
        operands.append(so_far)
        specs.append(pl.BlockSpec(memory_space=pl.ANY))
    return pl.pallas_call(
        input_back_kernel,
        grid=(1,),
        in_specs=specs,
        out_specs=[row_of(x, seq), full(1, model)],
        out_shape=[shape_of(x.shape, F32), shape_of((1, model), F32)],
        input_output_aliases=aliases,
        cost_estimate=pl.CostEstimate(
            flops=4 * tokens * model * w.shape[1],
            transcendentals=0,
            bytes_accessed=14 * tokens * model,
        ),
        compiler_params=params(),
        name="input_back",
    )(*operands)


def tp_other(values):
    return lax.ppermute(values, "tp", [(0, 1), (1, 0)])


def core_other(values):
    return lax.ppermute(values, "dp", [(i, i ^ 1) for i in range(lax.axis_size("dp"))])


def row_back(values, shift):
    rows = lax.axis_size("dp") // 2
    pairs = [(r * 2 + c, (r + shift) % rows * 2 + c) for r in range(rows) for c in range(2)]
    return lax.ppermute(values, "dp", pairs)


def earlier(values, shift):
    n = lax.axis_size("ctx")
    return lax.ppermute(values, "ctx", [(i, i + shift) for i in range(n - shift)])


def later(values, shift):
    n = lax.axis_size("ctx")
    return lax.ppermute(values, "ctx", [(i + shift, i) for i in range(n - shift)])


def tree_sum(terms):
    if len(terms) == 1:
        return terms[0]
    if len(terms) % 2:
        return terms[0] + tree_sum(terms[1:])
    return tree_sum(terms[0::2]) + tree_sum(terms[1::2])


def ring_sum(part):
    n = lax.axis_size("ctx")
    mine = part.astype(BF)
    terms = [mine]
    for shift in range(1, n):
        terms.append(lax.ppermute(mine, "ctx", [(i, (i + shift) % n) for i in range(n)]))
    return tree_sum([t.astype(F32) for t in terms])


def line_sum(part):
    n = lax.axis_size("ctx")
    half = n // 2
    me = lax.axis_index("ctx")
    for step in range(half - 1):
        pairs = [(step, step + 1), (n - 1 - step, n - 2 - step)]
        part = part + lax.ppermute(part.astype(BF), "ctx", pairs).astype(F32)
    mine = part.astype(BF)
    moved = lax.ppermute(mine, "ctx", [(half - 1, half), (half, half - 1)])
    total = (mine.astype(F32) + moved.astype(F32)).astype(BF)
    for step in reversed(range(half - 1)):
        pairs = [(step + 1, step), (n - 2 - step, n - 1 - step)]
        moved = lax.ppermute(total, "ctx", pairs)
        total = jnp.where((me == step) | (me == n - 1 - step), moved, total)
    return total.astype(F32)


def shards(
    block_input,
    positions,
    gain_attn,
    w_qkv,
    b_qkv,
    w_out,
    gain_mlp,
    w_gate,
    w_up,
    w_down,
    cotangent,
):
    seqs, tokens, model = block_input.shape
    heads_width = w_out.shape[1]
    n_ctx, n_dp = lax.axis_size("ctx"), lax.axis_size("dp")
    n_row = n_dp // 2
    me, my_dp = lax.axis_index("ctx"), lax.axis_index("dp")
    row, core = my_dp // 2, my_dp % 2
    first_token = me * tokens
    every = range(seqs)
    share = model // n_dp
    proj_qkv, proj_out = w_qkv[:, 0, :], w_out[0]
    other_out = tp_other(proj_out)
    other_qkv = tp_other(proj_qkv)
    gain_one, gain_two = gain_attn[None, :], gain_mlp[None, :]

    half = HD // 2
    freq = THETA ** (-(jnp.arange(half, dtype=F32) * 2.0) / HD)
    angle = positions.astype(F32)[:, None, :] * freq[None, :, None]
    cosine, sine = jnp.cos(angle), jnp.sin(angle)
    query_first = (first_token + jnp.arange(tokens, dtype=jnp.int32))[None, :] - positions
    counts = me - query_first[:, 0] // tokens + 1
    info = jnp.concatenate(
        [first_token[None], jnp.stack([counts, query_first[:, -1]], axis=1).reshape(-1)]
    ).astype(jnp.int32)
    query_first = query_first[:, None, :]
    rows_from = (row + jnp.arange(n_row, dtype=jnp.int32)) % n_row
    places = jnp.concatenate([rows_from * 2 + core, rows_from]).astype(jnp.int32)

    def for_other_core(turned):
        split = turned.reshape(n_row, 2, share, turned.shape[1])
        return core_other(lax.dynamic_index_in_dim(split, 1 - core, 1, keepdims=False))

    def blocks(turned):
        return turned.reshape(n_dp, share, turned.shape[1])

    def gradient(lefts, lefts_other, rights, rights_other, tile=512):
        own, *sent = weight_grad(places, lefts + lefts_other, rights + rights_other, tile)
        return own, sent

    def over_rows(own, sent):
        for shift in range(1, n_row):
            own = own + row_back(sent[shift - 1], shift).astype(F32)
        return own

    hidden_t, queries, key_value = project(
        block_input, gain_one, proj_qkv, b_qkv, cosine, sine, heads_width
    )
    pairs = [key_value] + [earlier(key_value, shift) for shift in range(1, n_ctx)]
    cot_t = jnp.swapaxes(cotangent, 1, 2)
    cot_other = [for_other_core(cot_t[i]) for i in every]
    hidden_other = [for_other_core(hidden_t[i]) for i in every]

    attended, lse = zip(*[attend(i, info, queries, pairs, query_first) for i in every])
    att_moved = [tp_other(a) for a in attended]
    middle, hid_t, acts, gates, ups, part, back = zip(
        *[
            mlp(
                i,
                block_input,
                attended[i],
                att_moved[i],
                proj_out,
                other_out,
                gain_two,
                cotangent,
                w_gate,
                w_up,
                w_down,
            )
            for i in every
        ]
    )
    back_moved = [tp_other(b) for b in back]
    part_moved = [tp_other(p) for p in part]
    output = jnp.stack(
        [
            (middle[i] + (part[i].astype(F32) + part_moved[i].astype(F32))).astype(BF)
            for i in every
        ]
    )
    hid_other = [for_other_core(h) for h in hid_t]
    hid_blocks = [blocks(h) for h in hid_t]
    acts_other, gates_other, ups_other = (
        [core_other(a) for a in group] for group in (acts, gates, ups)
    )
    down = gradient([blocks(cot_t[i]) for i in every], cot_other, list(acts), acts_other)
    gate = gradient(hid_blocks, hid_other, list(gates), gates_other)
    up = gradient(hid_blocks, hid_other, list(ups), ups_other)
    back_moved, down, gate, up = lax.optimization_barrier((back_moved, down, gate, up))
    down, gate, up = over_rows(*down), over_rows(*gate), over_rows(*up)
    grad_down, grad_gate, grad_up = line_sum(down).T, line_sum(gate), line_sum(up)

    results = [
        attend_back(
            i,
            info,
            back[i],
            back_moved[i],
            middle[i],
            cotangent,
            gain_two,
            proj_out,
            attended[i],
            queries,
            lse[i],
            query_first,
            cosine,
            sine,
            pairs,
        )
        for i in every
    ]
    grad_mid, grad_mid_t, gain_mlp_parts, grad_q, bias_q, grad_own = zip(*[r[:6] for r in results])
    grad_q_moved = [tp_other(g) for g in grad_q]
    pair_results = [
        pair_back(
            i,
            grad_own[i],
            [later(results[i][5 + shift], shift) for shift in range(1, n_ctx)],
            cosine,
            sine,
        )
        for i in every
    ]
    grad_kv, bias_kv = zip(*pair_results)
    grad_kv_moved = [tp_other(g) for g in grad_kv]

    mid_blocks = [blocks(g) for g in grad_mid_t]
    mid_other = [for_other_core(g) for g in grad_mid_t]
    hidden_blocks = [blocks(hidden_t[i]) for i in every]
    grad_out = over_rows(
        *gradient(mid_blocks, mid_other, list(attended), [core_other(a) for a in attended])
    )
    grad_out = ring_sum(grad_out).T[None]
    qkv_q = over_rows(
        *gradient(hidden_blocks, hidden_other, list(grad_q), [core_other(g) for g in grad_q])
    )
    qkv_kv = over_rows(
        *gradient(hidden_blocks, hidden_other, list(grad_kv), [core_other(g) for g in grad_kv])
    )
    grad_qkv = jnp.concatenate([ring_sum(qkv_q), ring_sum(qkv_kv)], axis=1)[:, None, :]

    grad_input, gain_attn_parts = None, []
    for i in every:
        grad_input, gain_part = input_back(
            i,
            grad_q[i],
            grad_q_moved[i],
            grad_kv[i],
            grad_kv_moved[i],
            proj_qkv,
            other_qkv,
            block_input,
            gain_one,
            grad_mid[i],
            grad_input,
        )
        gain_attn_parts.append(gain_part)

    def small_sum(values):
        values = values + core_other(values)
        values = tree_sum([values] + [row_back(values, shift) for shift in range(1, n_row)])
        ring = [
            lax.ppermute(values, "ctx", [(i, (i + shift) % n_ctx) for i in range(n_ctx)])
            for shift in range(1, n_ctx)
        ]
        return tree_sum([values] + ring)[0]

    small = small_sum(
        jnp.concatenate(
            [sum(gain_attn_parts), sum(gain_mlp_parts), sum(bias_q), sum(bias_kv)], axis=1
        )
    )

    def my_part(values):
        size = values.shape[0] // n_dp
        return lax.dynamic_slice_in_dim(values, my_dp * size, size)

    return (
        output,
        grad_input,
        my_part(small[:model]),
        grad_qkv,
        my_part(small[2 * model :])[None],
        grad_out,
        my_part(small[model : 2 * model]),
        grad_gate,
        grad_up,
        grad_down,
    )


def solution(mesh):
    in_specs = (
        P("dp", "ctx", None),
        P("dp", "ctx"),
        P(),
        P(None, "tp", None),
        P("tp", None),
        P("tp", None, None),
        P(),
        P(None, "tp"),
        P(None, "tp"),
        P("tp", None),
        P("dp", "ctx", None),
    )
    out_specs = (
        P("dp", "ctx", None),
        P("dp", "ctx", None),
        P("dp"),
        P("dp", "tp", None),
        P("tp", "dp"),
        P("tp", None, "dp"),
        P("dp"),
        P("dp", "tp"),
        P("dp", "tp"),
        P("tp", "dp"),
    )
    return jax.shard_map(shards, mesh=mesh, in_specs=in_specs, out_specs=out_specs, check_vma=False)
```

```python
import functools

import jax
import jax.numpy as jnp
from jax import lax
from jax.experimental import pallas as pl
from jax.experimental.pallas import tpu as pltpu
from jax.sharding import PartitionSpec as P


EPS = 1e-06
THETA = 1000000.0
SCALE = 0.125
NEGATIVE = -1e30
HD = 64
F32 = jnp.float32
BF = jnp.bfloat16
VMEM_LIMIT = 60 * 2**20


def shape_of(shape, dtype):
    return jax.ShapeDtypeStruct(shape, dtype)


def dot(a, b):
    return jnp.dot(a, b, preferred_element_type=F32)


def dot_nt(a, b):
    return lax.dot_general(a, b, (((1,), (1,)), ((), ())), preferred_element_type=F32)


def turn(rows, cosine, sine):
    half = rows.shape[0] // 2
    first, second = rows[:half], rows[half:]
    return jnp.concatenate([first * cosine - second * sine, second * cosine + first * sine], axis=0)


def inverse_rms(values):
    return lax.rsqrt(jnp.mean(values * values, axis=-1, keepdims=True) + EPS)


def norm_back(back, normed, scale, gain):
    upstream = back * gain
    inner = jnp.mean(upstream * normed, axis=-1, keepdims=True)
    return scale * (upstream - normed * inner)


def whole(a):
    return pl.BlockSpec(a.shape, lambda *_: (0,) * a.ndim)


def row_of(a, seq):
    return pl.BlockSpec((1,) + a.shape[1:], lambda *_: (seq,) + (0,) * (a.ndim - 1))


def full(*shape):
    return pl.BlockSpec(shape, lambda *_: (0,) * len(shape))


def params():
    return pltpu.CompilerParams(vmem_limit_bytes=VMEM_LIMIT)


def project_kernel(x_ref, gain_ref, w_ref, b_ref, cos_ref, sin_ref, hidden_ref, q_ref, kv_ref):
    x = x_ref[0].astype(F32)
    hidden = x * inverse_rms(x) * gain_ref[...]
    hidden_ref[0] = hidden.T.astype(BF)
    turned = (dot(hidden.astype(BF), w_ref[...]) + b_ref[...]).T
    cosine, sine = cos_ref[0], sin_ref[0]
    width = q_ref.shape[1]
    for start in range(0, width, HD):
        rows = slice(start, start + HD)
        q_ref[0, rows, :] = (turn(turned[rows], cosine, sine) * SCALE).astype(BF)
    keys = turn(turned[width : width + HD], cosine, sine)
    kv_ref[0] = jnp.concatenate([keys, turned[width + HD :]], axis=0).T.astype(BF)


def project(x, gain, w, b, cosine, sine, width):
    seqs, tokens, model = x.shape
    per = lambda r, c: pl.BlockSpec((1, r, c), lambda s: (s, 0, 0))
    half = cosine.shape[1]
    return pl.pallas_call(
        project_kernel,
        grid=(seqs,),
        in_specs=[
            per(tokens, model),
            whole(gain),
            whole(w),
            whole(b),
            per(half, tokens),
            per(half, tokens),
        ],
        out_specs=[per(model, tokens), per(width, tokens), per(tokens, 2 * HD)],
        out_shape=[
            shape_of((seqs, model, tokens), BF),
            shape_of((seqs, width, tokens), BF),
            shape_of((seqs, tokens, 2 * HD), BF),
        ],
        cost_estimate=pl.CostEstimate(
            flops=2 * seqs * tokens * model * w.shape[1],
            transcendentals=0,
            bytes_accessed=8 * seqs * tokens * model,
        ),
        compiler_params=params(),
        name="project",
    )(x, gain, w, b, cosine, sine)


def allowed_of(first_ref, place, back, tokens):
    shape = (tokens, tokens)
    key = lax.broadcasted_iota(jnp.int32, shape, 0) + (place - back * tokens)
    query = lax.broadcasted_iota(jnp.int32, shape, 1) + place
    return (key <= query) & (key >= first_ref[0])


def attend_kernel(n, seq, info_ref, q_ref, first_ref, *refs):
    pair_refs, (out_ref, lse_ref, pairs_ref, top_ref, total_ref, acc_ref) = refs[:n], refs[n:]
    tokens = q_ref.shape[2]
    heads = q_ref.shape[1] // HD
    place = info_ref[0]
    count, last_first = info_ref[1 + 2 * seq], info_ref[2 + 2 * seq]
    for s in range(n):
        pairs_ref[s] = pair_refs[s][0]
    top_ref[...] = jnp.full_like(top_ref, NEGATIVE)
    total_ref[...] = jnp.zeros_like(total_ref)
    acc_ref[...] = jnp.zeros_like(acc_ref)

    def block(back, masked):
        pair = pairs_ref[back]
        keys = pair[:, :HD]
        values = pair.T[HD:]
        ok = allowed_of(first_ref, place, back, tokens) if masked else None
        for h in range(heads):
            rows = slice(h * HD, (h + 1) * HD)
            scores = dot(keys, q_ref[0, rows, :])
            if masked:
                scores = jnp.where(ok, scores, NEGATIVE)
            old = top_ref[h : h + 1, :]
            new = jnp.maximum(old, jnp.max(scores, axis=0, keepdims=True))
            weights = jnp.exp(scores - new)
            factor = jnp.exp(old - new)
            top_ref[h : h + 1, :] = new
            total_ref[h : h + 1, :] = total_ref[h : h + 1, :] * factor + jnp.sum(
                weights, axis=0, keepdims=True
            )
            acc_ref[rows, :] = acc_ref[rows, :] * factor + dot(values, weights.astype(BF))

    @pl.loop(0, count)
    def _(back):
        masked = (back == 0) | (last_first > place - back * tokens)

        @pl.when(masked)
        def _():
            block(back, True)

        @pl.when(jnp.logical_not(masked))
        def _():
            block(back, False)

    lse_ref[...] = top_ref[...] + jnp.log(total_ref[...])
    for h in range(heads):
        rows = slice(h * HD, (h + 1) * HD)
        acc_ref[rows, :] = acc_ref[rows, :] / total_ref[h : h + 1, :]
    out_ref[...] = acc_ref[...].T.astype(BF)


def attend(seq, info, q, pairs, first):
    _, width, tokens = q.shape
    n = len(pairs)
    heads = width // HD
    pad = -(-heads // 8) * 8
    return pl.pallas_call(
        functools.partial(attend_kernel, n, seq),
        grid_spec=pltpu.PrefetchScalarGridSpec(
            num_scalar_prefetch=1,
            grid=(1,),
            in_specs=[row_of(q, seq), row_of(first, seq)] + [row_of(p, seq) for p in pairs],
            out_specs=[full(tokens, width), full(pad, tokens)],
            scratch_shapes=[
                pltpu.VMEM((n, tokens, 2 * HD), BF),
                pltpu.VMEM((pad, tokens), F32),
                pltpu.VMEM((pad, tokens), F32),
                pltpu.VMEM((width, tokens), F32),
            ],
        ),
        out_shape=[shape_of((tokens, width), BF), shape_of((pad, tokens), F32)],
        cost_estimate=pl.CostEstimate(
            flops=8 * tokens * tokens * width,
            transcendentals=2 * heads * tokens * tokens,
            bytes_accessed=16 * tokens * width,
        ),
        compiler_params=params(),
        name="attend",
    )(info, q, first, *pairs)


def attend_back_kernel(
    n,
    seq,
    info_ref,
    mine_ref,
    other_ref,
    middle_ref,
    cot_ref,
    gain_ref,
    w_ref,
    att_ref,
    q_ref,
    lse_ref,
    first_ref,
    cos_ref,
    sin_ref,
    *refs,
):
    pair_refs, refs = refs[:n], refs[n:]
    gmid_ref, gmid_t_ref, gain_out_ref, gq_ref, bias_ref, own_ref = refs[:6]
    sent_refs, refs = refs[6 : 6 + n - 1], refs[6 + n - 1 :]
    pairs_ref, sent_ref, gt_ref, qn_ref, gn_ref, term_ref, gacc_ref = refs
    tokens = q_ref.shape[2]
    heads = q_ref.shape[1] // HD
    place = info_ref[0]
    count, last_first = info_ref[1 + 2 * seq], info_ref[2 + 2 * seq]
    for s in range(n):
        pairs_ref[s] = pair_refs[s][0]

    middle = middle_ref[...]
    scale = inverse_rms(middle)
    normed = middle * scale
    back = mine_ref[...].astype(F32) + other_ref[...].astype(F32)
    gain_out_ref[...] = jnp.sum(back * normed, axis=0, keepdims=True)
    gmid = cot_ref[0].astype(F32) + norm_back(back, normed, scale, gain_ref[...])
    gmid_ref[...] = gmid
    gmid_t = gmid.T.astype(BF)
    gmid_t_ref[...] = gmid_t
    gt_ref[...] = dot(w_ref[...], gmid_t).astype(BF)
    att = att_ref[...].astype(F32).T
    for h in range(heads):
        rows = slice(h * HD, (h + 1) * HD)
        grad = gt_ref[rows, :].astype(F32)
        term_ref[h : h + 1, :] = jnp.sum(grad * att[rows], axis=0, keepdims=True)
        gn_ref[h] = grad.T.astype(BF)
        qn_ref[h] = q_ref[0, rows, :].astype(F32).T.astype(BF)
    gacc_ref[...] = jnp.zeros_like(gacc_ref)

    def block(back, masked):
        pair = pairs_ref[back]
        keys, values = pair[:, :HD], pair[:, HD:]
        keys_t = pair.T[:HD]
        ok = allowed_of(first_ref, place, back, tokens) if masked else None
        grad_key = jnp.zeros((tokens, HD), F32)
        grad_value = jnp.zeros((tokens, HD), F32)
        for h in range(heads):
            rows = slice(h * HD, (h + 1) * HD)
            scores = dot(keys, q_ref[0, rows, :])
            probs = jnp.exp(scores - lse_ref[h : h + 1, :])
            if masked:
                probs = jnp.where(ok, probs, 0.0)
            grad_probs = dot(values, gt_ref[rows, :])
            grad_scores = (probs * (grad_probs - term_ref[h : h + 1, :])).astype(BF)
            grad_value = grad_value + dot(probs.astype(BF), gn_ref[h])
            grad_key = grad_key + dot(grad_scores, qn_ref[h])
            gacc_ref[rows, :] = gacc_ref[rows, :] + dot(keys_t, grad_scores)
        return jnp.concatenate([grad_key, grad_value], axis=1)

    @pl.loop(0, n)
    def _(back):
        masked = (back == 0) | (last_first > place - back * tokens)

        @pl.when(back >= count)
        def _():
            sent_ref[back] = jnp.zeros((tokens, 2 * HD), F32)

        @pl.when((back < count) & masked)
        def _():
            sent_ref[back] = block(back, True)

        @pl.when((back < count) & jnp.logical_not(masked))
        def _():
            sent_ref[back] = block(back, False)

    own_ref[...] = sent_ref[0]
    for s in range(n - 1):
        sent_refs[s][...] = sent_ref[s + 1].astype(BF)
    cosine, sine = cos_ref[0], sin_ref[0]
    for h in range(heads):
        rows = slice(h * HD, (h + 1) * HD)
        gacc_ref[rows, :] = turn(gacc_ref[rows, :] * SCALE, cosine, -sine)
    out = gacc_ref[...].T
    gq_ref[...] = out.astype(BF)
    bias_ref[...] = jnp.sum(out, axis=0, keepdims=True)


def attend_back(seq, info, mine, other, middle, cot, gain, w, att, q, lse, first, cosine, sine, pairs):
    _, width, tokens = q.shape
    model = w.shape[1]
    n = len(pairs)
    heads = width // HD
    pad = lse.shape[0]
    pair = (tokens, 2 * HD)
    return pl.pallas_call(
        functools.partial(attend_back_kernel, n, seq),
        grid_spec=pltpu.PrefetchScalarGridSpec(
            num_scalar_prefetch=1,
            grid=(1,),
            in_specs=[
                whole(mine),
                whole(other),
                whole(middle),
                row_of(cot, seq),
                whole(gain),
                whole(w),
                whole(att),
                row_of(q, seq),
                whole(lse),
                row_of(first, seq),
                row_of(cosine, seq),
                row_of(sine, seq),
            ]
            + [row_of(p, seq) for p in pairs],
            out_specs=[
                full(tokens, model),
                full(model, tokens),
                full(1, model),
                full(tokens, width),
                full(1, width),
                full(*pair),
            ]
            + [full(*pair)] * (n - 1),
            scratch_shapes=[
                pltpu.VMEM((n,) + pair, BF),
                pltpu.VMEM((n,) + pair, F32),
                pltpu.VMEM((width, tokens), BF),
                pltpu.VMEM((heads, tokens, HD), BF),
                pltpu.VMEM((heads, tokens, HD), BF),
                pltpu.VMEM((pad, tokens), F32),
                pltpu.VMEM((width, tokens), F32),
            ],
        ),
        out_shape=[
            shape_of((tokens, model), F32),
            shape_of((model, tokens), BF),
            shape_of((1, model), F32),
            shape_of((tokens, width), BF),
            shape_of((1, width), F32),
            shape_of(pair, F32),
        ]
        + [shape_of(pair, BF)] * (n - 1),
        cost_estimate=pl.CostEstimate(
            flops=24 * tokens * tokens * width,
            transcendentals=2 * heads * tokens * tokens,
            bytes_accessed=16 * tokens * model,
        ),
        compiler_params=params(),
        name="attend_back",
    )(info, mine, other, middle, cot, gain, w, att, q, lse, first, cosine, sine, *pairs)


def mlp_kernel(
    total,
    places_ref,
    x_ref,
    mine_ref,
    other_ref,
    wo_ref,
    wx_ref,
    gain_ref,
    cot_ref,
    gate_ref,
    up_ref,
    down_ref,
    middle_ref,
    near_ref,
    far_ref,
    acts_ref,
    part_ref,
    back_ref,
    turned_ref,
    hidden_ref,
    acc_ref,
    bacc_ref,
):
    j = pl.program_id(0)

    @pl.when(j == 0)
    def _():
        middle = x_ref[0].astype(F32) + (
            dot(mine_ref[...], wo_ref[...]) + dot(other_ref[...], wx_ref[...])
        )
        middle_ref[...] = middle
        hidden = middle * inverse_rms(middle) * gain_ref[...]
        hidden_ref[...] = hidden.astype(BF)
        turned_ref[0] = hidden.T.astype(BF)
        turned_ref[1] = cot_ref[0].astype(F32).T.astype(BF)
        shares = near_ref.shape[1]
        size = near_ref.shape[2]
        for k in range(2):
            for i in range(shares):
                near = pl.multiple_of(places_ref[i] * size, 16)
                far = pl.multiple_of(places_ref[shares + i] * size, 16)
                near_ref[k, i] = turned_ref[k, pl.ds(near, size), :]
                far_ref[k, i] = turned_ref[k, pl.ds(far, size), :]
        acc_ref[...] = jnp.zeros_like(acc_ref)
        bacc_ref[...] = jnp.zeros_like(bacc_ref)

    tile = gate_ref.shape[1]
    wg, wu, wd = gate_ref[...], up_ref[...], down_ref[...]
    if total % tile:
        left = total - j * tile
        cols = lax.broadcasted_iota(jnp.int32, wg.shape, 1) < left
        wg, wu = jnp.where(cols, wg, jnp.zeros_like(wg)), jnp.where(cols, wu, jnp.zeros_like(wu))
        rows = lax.broadcasted_iota(jnp.int32, wd.shape, 0) < left
        wd = jnp.where(rows, wd, jnp.zeros_like(wd))
    hidden = hidden_ref[...]
    gate = dot(hidden, wg)
    up = dot(hidden, wu)
    grad_act = dot_nt(cot_ref[0], wd)
    sigma = 1.0 / (1.0 + jnp.exp(-gate))
    silu = gate * sigma
    act = (silu * up).astype(BF)
    gg = (grad_act * up * sigma * (1.0 + gate * (1.0 - sigma))).astype(BF)
    gu = (grad_act * silu).astype(BF)
    acts_ref[0] = act
    acts_ref[1] = gg
    acts_ref[2] = gu
    acc_ref[...] += dot(act, wd)
    bacc_ref[...] += dot_nt(gg, wg) + dot_nt(gu, wu)

    @pl.when(j == pl.num_programs(0) - 1)
    def _():
        part_ref[...] = acc_ref[...].astype(BF)
        back_ref[...] = bacc_ref[...].astype(BF)


def mlp(seq, places, shares, x, mine, other, wo, wx, gain, cot, wg, wu, wd, tile=512):
    n_row = places.shape[0] // 2
    _, tokens, model = x.shape
    ff = wg.shape[1]
    columns = pl.BlockSpec((model, tile), lambda j, p: (0, j))
    lefts = (2, n_row, shares, tokens)
    return pl.pallas_call(
        functools.partial(mlp_kernel, ff),
        grid_spec=pltpu.PrefetchScalarGridSpec(
            num_scalar_prefetch=1,
            grid=(pl.cdiv(ff, tile),),
            in_specs=[
            row_of(x, seq),
            whole(mine),
            whole(other),
            whole(wo),
            whole(wx),
            whole(gain),
            row_of(cot, seq),
            columns,
            columns,
            pl.BlockSpec((tile, model), lambda j, p: (j, 0)),
        ],
        out_specs=[
            full(tokens, model),
            full(*lefts),
            full(*lefts),
            pl.BlockSpec((3, tokens, tile), lambda j, p: (0, 0, j)),
            full(tokens, model),
            full(tokens, model),
        ],
        scratch_shapes=[
            pltpu.VMEM((2, model, tokens), BF),
            pltpu.VMEM((tokens, model), BF),
            pltpu.VMEM((tokens, model), F32),
            pltpu.VMEM((tokens, model), F32),
        ],
        ),
        out_shape=[
            shape_of((tokens, model), F32),
            shape_of(lefts, BF),
            shape_of(lefts, BF),
            shape_of((3, tokens, ff), BF),
            shape_of((tokens, model), BF),
            shape_of((tokens, model), BF),
        ],
        cost_estimate=pl.CostEstimate(
            flops=12 * tokens * model * ff,
            transcendentals=tokens * ff,
            bytes_accessed=6 * model * ff + 6 * tokens * ff,
        ),
        compiler_params=params(),
        name="mlp",
    )(places, x, mine, other, wo, wx, gain, cot, wg, wu, wd)


def weight_kernel(count, shares, pieces, *refs):
    lefts, rights, outs = refs[:count], refs[count : 2 * count], refs[2 * count :]
    for share in range(shares):
        total = None
        for k in range(count):
            part = dot(lefts[k][0, share], rights[k][0])
            total = part if total is None else total + part
        size = total.shape[0] // pieces
        for piece in range(pieces):
            out = outs[share * pieces + piece]
            out[...] = total[piece * size : (piece + 1) * size].astype(out.dtype)


def weight_grad(lefts, kind, rights, which, pieces, tile=512):
    count = len(lefts)
    _, shares, rows, tokens = lefts[0].shape
    ff = rights[0].shape[2]
    tile = min(tile, ff)
    left = pl.BlockSpec((1, shares, rows, tokens), lambda j: (kind, 0, 0, 0))
    cols = pl.BlockSpec((1, tokens, tile), lambda j: (which, 0, j))
    out = pl.BlockSpec((rows // pieces, tile), lambda j: (0, j))
    shape = (rows // pieces, ff)
    outs = pl.pallas_call(
        functools.partial(weight_kernel, count, shares, pieces),
        grid=(pl.cdiv(ff, tile),),
        in_specs=[left] * count + [cols] * count,
        out_specs=[out] * (shares * pieces),
        out_shape=[shape_of(shape, F32)] * pieces + [shape_of(shape, BF)] * ((shares - 1) * pieces),
        cost_estimate=pl.CostEstimate(
            flops=2 * count * shares * rows * tokens * ff,
            transcendentals=0,
            bytes_accessed=2 * count * tokens * ff + 6 * rows * ff,
        ),
        compiler_params=params(),
        name="weight_grad",
    )(*lefts, *rights)
    return [outs[k * pieces : (k + 1) * pieces] for k in range(shares)]


def share_kernel(kinds, places_ref, *refs):
    near_ref, far_ref = refs[-2:]
    shares, size = near_ref.shape[1], near_ref.shape[2]
    for kind, count in enumerate(kinds):
        start = 2 * sum(kinds[:kind])
        lefts, rights = refs[start : start + count], refs[start + count : start + 2 * count]
        for out_ref, base in ((near_ref, 0), (far_ref, shares)):
            for i in range(shares):
                total = None
                for left, right in zip(lefts, rights):
                    place = pl.multiple_of(places_ref[base + i] * size, 16)
                    part = dot(left[0, pl.ds(place, size), :], right[...])
                    total = part if total is None else total + part
                out_ref[kind, i] = total


def share_grads(places, share, groups):
    shares = places.shape[0] // 2
    operands, specs = [], []
    for group in groups:
        for left, index, _ in group:
            operands.append(left)
            specs.append(row_of(left, index))
        for _, _, right in group:
            operands.append(right)
            specs.append(whole(right))
    width = groups[0][0][2].shape[1]
    shape = (len(groups), shares, share, width)
    return pl.pallas_call(
        functools.partial(share_kernel, [len(g) for g in groups]),
        grid_spec=pltpu.PrefetchScalarGridSpec(
            num_scalar_prefetch=1,
            grid=(1,),
            in_specs=specs,
            out_specs=[full(*shape), full(*shape)],
        ),
        out_shape=[shape_of(shape, F32), shape_of(shape, F32)],
        cost_estimate=pl.CostEstimate(
            flops=4 * len(operands) * shares * share * width * operands[0].shape[-1],
            transcendentals=0,
            bytes_accessed=sum(o.size * 2 for o in operands),
        ),
        compiler_params=params(),
        name="share_grads",
    )(places, *operands)


def pair_back_kernel(own_ref, cos_ref, sin_ref, *refs):
    moved, out_ref, bias_ref = refs[:-2], refs[-2], refs[-1]
    total = own_ref[...]
    for ref in moved:
        total = total + ref[...].astype(F32)
    turned = total.T
    keys = turn(turned[:HD], cos_ref[0], -sin_ref[0])
    total = jnp.concatenate([keys, turned[HD:]], axis=0).T
    out_ref[...] = total.astype(BF)
    bias_ref[...] = jnp.sum(total, axis=0, keepdims=True)


def pair_back(seq, own, moved, cosine, sine):
    return pl.pallas_call(
        pair_back_kernel,
        grid=(1,),
        in_specs=[whole(own), row_of(cosine, seq), row_of(sine, seq)] + [whole(m) for m in moved],
        out_specs=[full(*own.shape), full(1, own.shape[1])],
        out_shape=[shape_of(own.shape, BF), shape_of((1, own.shape[1]), F32)],
        compiler_params=params(),
        name="pair_back",
    )(own, cosine, sine, *moved)


def input_back_kernel(
    gq_ref, gqx_ref, gkv_ref, gkvx_ref, w_ref, wx_ref, x_ref, gain_ref, gmid_ref, *refs
):
    out_ref, gain_out_ref = refs[-2:]
    width = gq_ref.shape[1]

    def back_of(q_ref, kv_ref, weights):
        return dot_nt(q_ref[...], weights[:, :width]) + dot_nt(kv_ref[...], weights[:, width:])

    back = back_of(gq_ref, gkv_ref, w_ref[...]) + back_of(gqx_ref, gkvx_ref, wx_ref[...])
    x = x_ref[0].astype(F32)
    scale = inverse_rms(x)
    normed = x * scale
    gain_out_ref[...] = jnp.sum(back * normed, axis=0, keepdims=True)
    out_ref[0] = gmid_ref[...] + norm_back(back, normed, scale, gain_ref[...])


def input_back(seq, gq, gqx, gkv, gkvx, w, wx, x, gain, gmid, so_far):
    _, tokens, model = x.shape
    operands = [gq, gqx, gkv, gkvx, w, wx, x, gain, gmid]
    specs = [whole(a) for a in operands]
    specs[6] = row_of(x, seq)
    aliases = {}
    if so_far is not None:
        aliases = {len(operands): 0}
        operands.append(so_far)
        specs.append(pl.BlockSpec(memory_space=pl.ANY))
    return pl.pallas_call(
        input_back_kernel,
        grid=(1,),
        in_specs=specs,
        out_specs=[row_of(x, seq), full(1, model)],
        out_shape=[shape_of(x.shape, F32), shape_of((1, model), F32)],
        input_output_aliases=aliases,
        cost_estimate=pl.CostEstimate(
            flops=4 * tokens * model * w.shape[1],
            transcendentals=0,
            bytes_accessed=14 * tokens * model,
        ),
        compiler_params=params(),
        name="input_back",
    )(*operands)


def tp_other(values):
    return lax.ppermute(values, "tp", [(0, 1), (1, 0)])


def core_other(values):
    return lax.ppermute(values, "dp", [(i, i ^ 1) for i in range(lax.axis_size("dp"))])


def row_back(values, shift):
    rows = lax.axis_size("dp") // 2
    pairs = [(r * 2 + c, (r + shift) % rows * 2 + c) for r in range(rows) for c in range(2)]
    return lax.ppermute(values, "dp", pairs)


def earlier(values, shift):
    n = lax.axis_size("ctx")
    return lax.ppermute(values, "ctx", [(i, i + shift) for i in range(n - shift)])


def later(values, shift):
    n = lax.axis_size("ctx")
    return lax.ppermute(values, "ctx", [(i + shift, i) for i in range(n - shift)])


def doubling_sum(part, axis, size, stride, dtype):
    n = lax.axis_size(axis)
    bit = 1
    while bit < size:
        mine = part.astype(dtype)
        pairs = [(i, (i // stride ^ bit) * stride + i % stride) for i in range(n)]
        part = mine.astype(F32) + lax.ppermute(mine, axis, pairs).astype(F32)
        bit *= 2
    return part


def line_sum(part):
    n = lax.axis_size("ctx")
    half = n // 2
    me = lax.axis_index("ctx")
    for step in range(half - 1):
        pairs = [(step, step + 1), (n - 1 - step, n - 2 - step)]
        moved = lax.ppermute(part.astype(BF), "ctx", pairs)
        part = part + moved.astype(F32)
    mine = part.astype(BF)
    moved = lax.ppermute(mine, "ctx", [(half - 1, half), (half, half - 1)])
    total = (mine.astype(F32) + moved.astype(F32)).astype(BF)
    for step in reversed(range(half - 1)):
        pairs = [(step + 1, step), (n - 2 - step, n - 1 - step)]
        moved = lax.ppermute(total, "ctx", pairs)
        total = jnp.where((me == step) | (me == n - 1 - step), moved, total)
    return total.astype(F32)


def layer(
    block_input,
    positions,
    gain_attn,
    w_qkv,
    b_qkv,
    w_out,
    gain_mlp,
    w_gate,
    w_up,
    w_down,
    cotangent,
):
    seqs, tokens, model = block_input.shape
    heads_width = w_out.shape[1]
    n_ctx, n_dp = lax.axis_size("ctx"), lax.axis_size("dp")
    n_row = n_dp // 2
    me, my_dp = lax.axis_index("ctx"), lax.axis_index("dp")
    row, core = my_dp // 2, my_dp % 2
    first_token = me * tokens
    every = range(seqs)
    share = model // n_dp
    proj_qkv, proj_out = w_qkv[:, 0, :], w_out[0]
    other_out = tp_other(proj_out)
    other_qkv = tp_other(proj_qkv)
    gain_one, gain_two = gain_attn[None, :], gain_mlp[None, :]

    half = HD // 2
    freq = THETA ** (-(jnp.arange(half, dtype=F32) * 2.0) / HD)
    angle = positions.astype(F32)[:, None, :] * freq[None, :, None]
    cosine, sine = jnp.cos(angle), jnp.sin(angle)
    query_first = (first_token + jnp.arange(tokens, dtype=jnp.int32))[None, :] - positions
    counts = me - query_first[:, 0] // tokens + 1
    info = jnp.concatenate(
        [first_token[None], jnp.stack([counts, query_first[:, -1]], axis=1).reshape(-1)]
    ).astype(jnp.int32)
    query_first = query_first[:, None, :]
    rows_from = (row + jnp.arange(n_row, dtype=jnp.int32)) % n_row
    places = jnp.concatenate([rows_from * 2 + core, rows_from * 2 + 1 - core]).astype(jnp.int32)

    hidden_t, queries, key_value = project(
        block_input, gain_one, proj_qkv, b_qkv, cosine, sine, heads_width
    )
    pairs = [key_value] + [earlier(key_value, shift) for shift in range(1, n_ctx)]
    attended, lse, att_moved = [], [], []
    for i in every:
        out, log = attend(i, info, queries, pairs, query_first)
        attended.append(out)
        lse.append(log)
        att_moved.append(tp_other(out))
    middle, near, far, acts, part, back = [], [], [], [], [], []
    for i in every:
        outs = mlp(
            i,
            places,
            share,
            block_input,
            attended[i],
            att_moved[i],
            proj_out,
            other_out,
            gain_two,
            cotangent,
            w_gate,
            w_up,
            w_down,
        )
        for group, out in zip((middle, near, far, acts, part, back), outs):
            group.append(out)
    back_moved, part_moved, lefts, rights = [], [], list(near), list(acts)
    for i in every:
        back_moved.append(tp_other(back[i]))
        part_moved.append(tp_other(part[i]))
        lefts.append(core_other(far[i]))
        rights.append(core_other(acts[i]))
    output = jnp.stack(
        [
            (middle[i] + (part[i].astype(F32) + part_moved[i].astype(F32))).astype(BF)
            for i in every
        ]
    )
    pieces = 2 if share % 32 == 0 else 1
    totals = []
    for kind, which in ((1, 0), (0, 1), (0, 2)):
        owns, *sents = weight_grad(lefts, kind, rights, which, pieces)
        total = []
        for piece, own in enumerate(owns):
            for shift in range(1, n_row):
                moved = row_back(sents[shift - 1][piece], shift)
                own = own + moved.astype(F32)
            total.append(line_sum(own))
        totals.append(jnp.concatenate(total, axis=0))
    grad_down, grad_gate, grad_up = totals[0].T, totals[1], totals[2]

    results = []
    for i in every:
        results.append(
            attend_back(
                i,
                info,
                back[i],
                back_moved[i],
                middle[i],
                cotangent,
                gain_two,
                proj_out,
                attended[i],
                queries,
                lse[i],
                query_first,
                cosine,
                sine,
                pairs,
            )
        )
    grad_mid, grad_mid_t, gain_mlp_parts, grad_q, bias_q, grad_own = zip(*[r[:6] for r in results])
    grad_q_moved = [tp_other(g) for g in grad_q]
    grad_kv, bias_kv = zip(
        *[
            pair_back(
                i,
                grad_own[i],
                [later(results[i][5 + shift], shift) for shift in range(1, n_ctx)],
                cosine,
                sine,
            )
            for i in every
        ]
    )
    grad_kv_moved = [tp_other(g) for g in grad_kv]

    def summed(groups):
        mine, theirs = share_grads(places, share, groups)
        total = mine + core_other(theirs)
        own = total[:, 0]
        for shift in range(1, n_row):
            own = own + row_back(total[:, shift].astype(BF), shift).astype(F32)
        return doubling_sum(own, "ctx", n_ctx, 1, BF)

    grad_out, qkv_q = summed(
        [
            [(grad_mid_t[i][None], 0, attended[i]) for i in every],
            [(hidden_t, i, grad_q[i]) for i in every],
        ],
    )
    grad_out = grad_out.T[None]
    (qkv_kv,) = summed([[(hidden_t, i, grad_kv[i]) for i in every]])
    grad_qkv = jnp.concatenate([qkv_q, qkv_kv], axis=1)[:, None, :]

    grad_input, gain_attn_parts = None, []
    for i in every:
        grad_input, gain_part = input_back(
            i,
            grad_q[i],
            grad_q_moved[i],
            grad_kv[i],
            grad_kv_moved[i],
            proj_qkv,
            other_qkv,
            block_input,
            gain_one,
            grad_mid[i],
            grad_input,
        )
        gain_attn_parts.append(gain_part)

    small = jnp.concatenate(
        [sum(gain_attn_parts), sum(gain_mlp_parts), sum(bias_q), sum(bias_kv)], axis=1
    )
    small = small + core_other(small)
    small = doubling_sum(small, "dp", n_row, 2, F32)
    small = doubling_sum(small, "ctx", n_ctx, 1, F32)[0]

    def my_part(values):
        size = values.shape[0] // n_dp
        return lax.dynamic_slice_in_dim(values, my_dp * size, size)

    return (
        output,
        grad_input,
        my_part(small[:model]),
        grad_qkv,
        my_part(small[2 * model :])[None],
        grad_out,
        my_part(small[model : 2 * model]),
        grad_gate,
        grad_up,
        grad_down,
    )


def solution(mesh):
    in_specs = (
        P("dp", "ctx", None),
        P("dp", "ctx"),
        P(),
        P(None, "tp", None),
        P("tp", None),
        P("tp", None, None),
        P(),
        P(None, "tp"),
        P(None, "tp"),
        P("tp", None),
        P("dp", "ctx", None),
    )
    out_specs = (
        P("dp", "ctx", None),
        P("dp", "ctx", None),
        P("dp"),
        P("dp", "tp", None),
        P("tp", "dp"),
        P("tp", None, "dp"),
        P("dp"),
        P("dp", "tp"),
        P("dp", "tp"),
        P("tp", "dp"),
    )
    return jax.shard_map(layer, mesh=mesh, in_specs=in_specs, out_specs=out_specs, check_vma=False)
```
